256 devices in a mesh: row: 16 (over x, y), col: 16 (over z, core).
Axes of the slice: x: 4, y: 4, z: 8, core: 2. Of those that a mesh axis runs over, the one named last changes fastest.
Arguments:
- values: bfloat16 [8192, 8192], P('row', 'col'), may hold values from 0.0001296997 to 0.12988281
- tile_mask: int32 [64, 64], P('row', 'col'), may hold values 0 or 1
- keep_mask: int32 [64, 64], P('row', 'col'), may hold values 0 or 1
- thr_index: int32 [8192], P('col'), may hold values from 0 to 9
Outputs:
- expanded: bfloat16 [8192, 8192], P('row', 'col')
The draws below stay inside these ranges and needn't reach their ends.
All inputs are finite; a program needn't handle non-finite values. No bound on the sum of `tile_mask` or of `keep_mask` on one device may be relied on, other than what follows from the above.
Results may differ from the reference program's by a relative error of at most 0.0004.
Values may be sent and summed in bfloat16 or wider, within the bound.
A program may use at most 64 MiB of HBM per device.

```python
import math
import jax
import jax.numpy as jnp

TB = 128
NT = 64
ORDER = 8192


def touch_ends(values, stream_key, smallest, largest):
    spot = [jax.random.randint(jax.random.fold_in(stream_key, axis), (), 0, length) for axis, length in enumerate(values.shape)]
    longest = values.shape.index(max(values.shape))
    neighbour = spot[:longest] + [(spot[longest] + 1) % values.shape[longest]] + spot[longest + 1:]
    return values.at[tuple(spot)].set(smallest).at[tuple(neighbour)].set(largest)


def levels(stream_key, extent, shards, least, largest):
    level = 1.0
    for dim, shards_of in shards:
        draws = jax.random.uniform(jax.random.fold_in(jax.random.fold_in(stream_key, 6), dim), (shards_of,), jnp.float32, least / len(shards), largest / len(shards))
        level = level * jnp.repeat(jnp.exp(draws), extent[dim] // shards_of).reshape((-1,) + (1,) * (len(extent) - 1 - dim))
    return level


def setup_inputs(seed: int = 0) -> dict:
    seeds = jax.random.split(jax.random.key(seed), 5)
    values = jnp.clip(jnp.exp(math.log(0.12988281) - 6.909166 * jax.random.uniform(seeds[0], (ORDER, ORDER), jnp.float32) ** levels(seeds[0], (ORDER, ORDER), ((0, 16), (1, 16)), -0.2, 0.2)), 0.0001296997, 0.12988281).astype(jnp.bfloat16)
    tile_mask = touch_ends((jax.random.randint(seeds[1], (NT, NT), 0, 2) < 1).astype(jnp.int32), jax.random.fold_in(seeds[1], 1), 0, 1)
    keep_mask = touch_ends((jax.random.randint(seeds[2], (NT, NT), 0, 4) < 3).astype(jnp.int32), jax.random.fold_in(seeds[2], 1), 0, 1)
    thr_index = touch_ends(jax.random.randint(seeds[3], (ORDER,), 0, 10), jax.random.fold_in(seeds[3], 1), 0, 9).astype(jnp.int32)
    return {"values": values, "tile_mask": tile_mask, "keep_mask": keep_mask, "thr_index": thr_index}


def reference(values, tile_mask, keep_mask, thr_index):
    matrix = (values.reshape(NT, TB, NT, TB) * tile_mask[:, None, :, None].astype(jnp.bfloat16)).reshape(ORDER, ORDER)
    product = jnp.dot(matrix, matrix, preferred_element_type=jnp.float32)
    col_means = jnp.sum(product, axis=0) / ORDER
    thresholds = 0.125 * thr_index.astype(jnp.float32)
    kept_cells = jnp.broadcast_to(keep_mask[:, None, :, None].astype(jnp.float32), (NT, TB, NT, TB)).reshape(ORDER, ORDER)
    pruned = jnp.maximum(product - thresholds * col_means, 0.0) * kept_cells
    col_totals = jnp.sum(pruned, axis=0) / ORDER
    return (pruned / jnp.maximum(col_totals, 0.1)).astype(jnp.bfloat16)
```

```python
import functools

import jax
import jax.numpy as jnp
from jax import lax
from jax.experimental import pallas as pl
from jax.experimental.pallas import tpu as pltpu
from jax.sharding import PartitionSpec as P

TB = 128
CORES = 2
SIDE = 4
CHIPS = 8
CHUNKS = 4
LAST = 10
EXTRA = 16
LINKS = ((1, 0), (-1, 0), (0, 1), (0, -1))

ORDER = (
    ((0, 0), (1, 0), (2, 0), (3, 0), (0, 4), (2, 3), (3, 3), (2, 4), (2, 1), (3, 1), (2, 2), (3, 2), (2, 5), (2, 7), (2, 6)),
    ((1, 0), (0, 0), (3, 0), (2, 0), (1, 12), (3, 1), (2, 1), (3, 12), (3, 3), (2, 3), (3, 2), (2, 2), (3, 13), (3, 15), (3, 14)),
    ((2, 0), (3, 0), (0, 0), (1, 0), (2, 1), (0, 12), (1, 12), (0, 4), (0, 1), (1, 4), (0, 8), (0, 13), (1, 8), (0, 5), (0, 9)),
    ((3, 0), (2, 0), (1, 0), (0, 0), (3, 3), (1, 4), (0, 4), (1, 12), (1, 3), (0, 12), (1, 8), (1, 15), (1, 7), (0, 8), (1, 11)),
)
SLOTS = len(ORDER[0])
Z_ORDER = (
    tuple((c, 0) for c in (0, 1, 2, 3)) + tuple((c, 1) for c in (0, 1, 2, 3))
    + tuple((c, 2) for c in (0, 1, 2, 3)) + ((0, 3), (1, 3)),
    tuple((c, 0) for c in (2, 3, 0, 1)) + tuple((c, 1) for c in (2, 3, 0, 1))
    + tuple((c, 2) for c in (2, 3, 0, 1)) + ((2, 3), (3, 3)),
)
Z_SLOTS = len(Z_ORDER[0])
AHEAD = 3
POINTS = (7, 9, 11, 12, 13)


def shift(place, link):
    dx, dy = LINKS[link]
    return (place // SIDE + dx) % SIDE * SIDE + (place % SIDE + dy) % SIDE


def arrivals():
    xy = {(c, shift(p, n)): s for n in range(4) for s, (c, p) in enumerate(ORDER[n])}
    z = {}
    for n, sign in ((0, 1), (1, -1)):
        for s, (c, hop) in enumerate(Z_ORDER[n]):
            z[c, sign * (hop + 1) % CHIPS] = s
    return xy, z


XY_AT, Z_AT = arrivals()
BLOCK_AT = {p: max(XY_AT[c, p] for c in range(CHUNKS)) for p in range(1, SIDE * SIDE)} | {0: 0}
NEAR_AT = [0] + [max(Z_AT[c, d] for c in range(CHUNKS) for d in (h, CHIPS - h)) for h in range(1, CHIPS // 2 + 1)]


def kernel(
    v_hbm, tile_hbm, keep_hbm, thr_hbm, acc, scale_ref,
    row_panel, col_panel, loaded, tile_ref, keep_ref, thr_ref, colsum, stats, sums, psum,
    xy_send, xy_recv, z_send, z_recv, pair_send, pair_recv,
    small_send, small_recv, load_sem, hello,
):
    rows, cols = v_hbm.shape
    part = rows // CHUNKS
    order = rows * SIDE * SIDE
    me_row, me_col = lax.axis_index("row"), lax.axis_index("col")
    x, y = me_row // SIDE, me_row % SIDE
    z, core = me_col // CORES, me_col % CORES

    def xy_device(dx, dy):
        return {"row": (x + dx + SIDE) % SIDE * SIDE + (y + dy + SIDE) % SIDE}

    def z_device(dz, lane=0):
        return {"col": (z + dz + CHIPS) % CHIPS * CORES + (core if lane == 0 else 1 - core)}

    neighbours = [xy_device(*link) for link in LINKS] + [z_device(1), z_device(-1), z_device(0, 1)]
    barrier = pltpu.get_barrier_semaphore()
    for device in neighbours:
        pl.semaphore_signal(barrier, inc=1, device_id=device)

    def load(q):
        spot = pl.ds(q * part, part)
        return pltpu.make_async_copy(v_hbm.at[spot], loaded.at[spot], load_sem.at[q])

    masks = (
        pltpu.make_async_copy(tile_hbm, tile_ref, load_sem.at[CHUNKS]),
        pltpu.make_async_copy(keep_hbm, keep_ref, load_sem.at[CHUNKS + 1]),
        pltpu.make_async_copy(thr_hbm, thr_ref, load_sem.at[CHUNKS + 2]),
    )
    masks[0].start()
    for q in range(CHUNKS):
        load(q).start()
    masks[1].start()
    masks[2].start()

    masks[0].wait()
    stored = tile_ref[...].astype(jnp.float32)
    for q in range(CHUNKS):
        load(q).wait()
        for lo in range(q * part, (q + 1) * part, min(part, TB)):
            for b in range(cols // TB):
                r, c = slice(lo, lo + min(part, TB)), slice(b * TB, (b + 1) * TB)
                i = lo // TB
                factor = jnp.broadcast_to(stored[i : i + 1, b : b + 1], (min(part, TB), TB))
                tile = (loaded[r, c].astype(jnp.float32) * factor).astype(jnp.bfloat16)
                row_panel[0, r, c] = tile
                col_panel[r, c] = tile

    pl.semaphore_wait(barrier, len(neighbours))

    def xy_copy(c, place, n):
        to = shift(place, n)
        return pltpu.make_async_remote_copy(
            src_ref=col_panel.at[pl.ds(place * rows + c * part, part)],
            dst_ref=col_panel.at[pl.ds(to * rows + c * part, part)],
            send_sem=xy_send.at[n], recv_sem=xy_recv.at[to, c],
            device_id=neighbours[n],
        )

    def z_copy(c, hop, n):
        sign = 1 - 2 * n
        spot = pl.ds(c * part, part)
        to = sign * (hop + 1) % CHIPS
        return pltpu.make_async_remote_copy(
            src_ref=row_panel.at[sign * hop % CHIPS * CORES, spot],
            dst_ref=row_panel.at[to * CORES, spot],
            send_sem=z_send.at[n], recv_sem=z_recv.at[to, c],
            device_id=neighbours[4 + n],
        )

    def pair_copy(c, dz):
        spot = pl.ds(c * part, part)
        return pltpu.make_async_remote_copy(
            src_ref=row_panel.at[dz * CORES, spot], dst_ref=row_panel.at[dz * CORES + 1, spot],
            send_sem=pair_send.at[0], recv_sem=pair_recv.at[dz, c],
            device_id=neighbours[6],
        )

    def send(s):
        for n in range(4):
            if s < SLOTS:
                xy_copy(*ORDER[n][s], n).start()
            if n < 2 and s < Z_SLOTS:
                z_copy(*Z_ORDER[n][s], n).start()

    for s in range(AHEAD):
        send(s)
    for c in range(CHUNKS):
        pair_copy(c, 0).start()

    def greet(k):
        for device in neighbours:
            pl.semaphore_signal(hello.at[k], inc=1, device_id=device)
        pl.semaphore_wait(hello.at[k], len(neighbours))

    total = jnp.zeros((1, cols), jnp.float32)
    for lo in range(0, rows, TB):
        block = col_panel[lo : lo + TB].astype(jnp.float32)
        total += jnp.sum(block, axis=0, keepdims=True)
    colsum[0] = total
    for k in range(3):
        greet(k)

    def spread(buffer, k, count, device):
        def copy(d):
            return pltpu.make_async_remote_copy(
                src_ref=buffer.at[0], dst_ref=buffer.at[d],
                send_sem=small_send.at[k], recv_sem=small_recv.at[k], device_id=device(d),
            )

        everything = pltpu.make_async_remote_copy(
            src_ref=buffer.at[pl.ds(1, count - 1)], dst_ref=buffer.at[pl.ds(1, count - 1)],
            send_sem=small_send.at[k], recv_sem=small_recv.at[k], device_id=neighbours[6],
        )
        return [copy(d) for d in range(1, count)], everything

    def by_row(d):
        return xy_device(d // SIDE, d % SIDE)

    def by_col(d):
        return z_device(d // CORES, d % CORES)

    column_sums, column_sums_all = spread(colsum, 0, SIDE * SIDE, by_row)
    for copy in column_sums:
        copy.start()
    greet(3)
    acc[...] = jnp.zeros((rows, cols), jnp.float32)
    psum[...] = jnp.zeros((EXTRA, cols), jnp.float32)

    block_sums, block_sums_all = spread(stats, 1, CHIPS * CORES, by_col)

    def send_block_sums():
        column_sums_all.wait_recv()
        column_sums_all.wait_send()
        total = colsum[0]
        for i in range(1, SIDE * SIDE):
            total += colsum[i]
        stats[0] = total
        for copy in block_sums:
            copy.start()

    def take_block_sums():
        block_sums_all.wait_recv()
        block_sums_all.wait_send()
        line = lax.broadcasted_iota(jnp.int32, (EXTRA, cols), 0)

        @pl.loop(0, CHIPS * CORES)
        def _(i):
            rest, spot = stats[i], jnp.zeros((EXTRA, cols), jnp.float32)
            for k in range(3):
                term = rest.astype(jnp.bfloat16).astype(jnp.float32)
                rest = rest - term
                spot = jnp.where(line == k, jnp.broadcast_to(term, (EXTRA, cols)), spot)
            row_panel[i, rows:] = spot.astype(jnp.bfloat16)

    def inner(j):
        k = (x - j // SIDE + SIDE) % SIDE * SIDE + (y - j % SIDE + SIDE) % SIDE
        dz = (z - k // CORES + CHIPS) % CHIPS
        lane = (core + k) % CORES
        return dz, lane

    def have(j, step):
        dz, lane = inner(j)
        here = j == 0
        for p in range(1, SIDE * SIDE):
            if BLOCK_AT[p] <= step:
                here = here | (j == p)
        near = [-1, -1]
        for h in range(CHIPS // 2 + 1):
            for side in range(CORES):
                if NEAR_AT[h] + side <= step:
                    near[side] = h
        there = None
        for side in range(CORES):
            one = (lane == side) & ((dz <= near[side]) | (dz >= CHIPS - near[side]))
            there = one if there is None else there | one
        return here & there

    def compute(step, before):
        @pl.loop(0, SIDE * SIDE)
        def _(j):
            go = have(j, step) if step is not None else (j != LAST)
            if before is not None:
                go = go & jnp.logical_not(have(j, before))

            @pl.when(go)
            def _():
                dz, lane = inner(j)
                block = col_panel[pl.ds(pl.multiple_of(j * rows, rows), rows)]
                term = jnp.dot(row_panel[dz * CORES + lane], block, preferred_element_type=jnp.float32)
                acc[...] += term[:rows]
                psum[...] += term[rows:]

    def take_xy(s):
        for n in range(4):
            c, place = ORDER[n][s]
            xy_copy(c, place, n).wait_recv()

    def take_z(s):
        for n in range(2):
            if s < Z_SLOTS:
                c, hop = Z_ORDER[n][s]
                z_copy(c, hop, n).wait_recv()
                pair_copy(c, (1 - 2 * n) * (hop + 1) % CHIPS).start()

    def take_pair(s):
        if s == 0:
            for c in range(CHUNKS):
                pair_copy(c, 0).wait_recv()
        elif s <= Z_SLOTS:
            for n in range(2):
                c, hop = Z_ORDER[n][s - 1]
                pair_copy(c, (1 - 2 * n) * (hop + 1) % CHIPS).wait_recv()

    before = None
    for s in range(SLOTS):
        take_z(s)
        take_pair(s)
        if s < SLOTS - 1:
            take_xy(s)
            send(s + AHEAD)
        if s == 3:
            send_block_sums()
        if s == 6:
            take_block_sums()
        if s in POINTS:
            compute(s, before)
            before = s
    compute(None, before)

    masks[1].wait()
    masks[2].wait()
    kept = keep_ref[...].astype(jnp.float32)
    level = 0.125 * thr_ref[...].astype(jnp.float32)
    take_xy(SLOTS - 1)
    dz, lane = inner(LAST)
    slot = dz * CORES + lane
    block = col_panel[LAST * rows : (LAST + 1) * rows]
    lines = psum[...] + jnp.dot(row_panel[slot, rows:], block, preferred_element_type=jnp.float32)
    cut = level * ((lines[2:3] + lines[1:2] + lines[0:1]) / order)
    parts = [jnp.zeros((1, TB), jnp.float32) for _ in range(cols // TB)]
    for lo in range(0, rows, TB):
        term = jnp.dot(row_panel[slot, lo : lo + TB], block, preferred_element_type=jnp.float32)
        for b in range(cols // TB):
            r, c = slice(lo, lo + TB), slice(b * TB, (b + 1) * TB)
            keep = jnp.broadcast_to(kept[lo // TB : lo // TB + 1, b : b + 1], (TB, TB))
            pruned = jnp.maximum(acc[r, c] + term[:, c] - cut[:, c], 0.0) * keep
            acc[r, c] = pruned
            parts[b] += jnp.sum(pruned, axis=0, keepdims=True)
    sums[0] = jnp.concatenate(parts, axis=1)

    totals, totals_all = spread(sums, 2, SIDE * SIDE, by_row)
    for copy in totals:
        copy.start()

    for n in range(4):
        spot = col_panel.at[pl.ds(0, SLOTS * part)]
        pltpu.make_async_remote_copy(
            src_ref=spot, dst_ref=spot, send_sem=xy_send.at[n], recv_sem=xy_send.at[n], device_id=neighbours[n]
        ).wait_send()
    for n in range(2):
        spot = col_panel.at[pl.ds(0, Z_SLOTS * part)]
        pltpu.make_async_remote_copy(
            src_ref=spot, dst_ref=spot, send_sem=z_send.at[n], recv_sem=z_send.at[n], device_id=neighbours[4 + n]
        ).wait_send()
    spot = col_panel.at[pl.ds(0, CHIPS * rows)]
    pltpu.make_async_remote_copy(
        src_ref=spot, dst_ref=spot, send_sem=pair_send.at[0], recv_sem=pair_send.at[0], device_id=neighbours[6]
    ).wait_send()

    totals_all.wait_send()
    totals_all.wait_recv()
    total = sums[0]
    for i in range(1, SIDE * SIDE):
        total += sums[i]
    scale_ref[...] = 1.0 / jnp.maximum(total / order, 0.1)


def on_device(values, tile_mask, keep_mask, thr_index):
    rows, cols = values.shape
    dma, plain = pltpu.SemaphoreType.DMA, pltpu.SemaphoreType.REGULAR
    vmem, anywhere = pl.BlockSpec(memory_space=pltpu.VMEM), pl.BlockSpec(memory_space=pl.ANY)
    blocks = SIDE * SIDE
    pruned, scale = pl.pallas_call(
        kernel,
        out_shape=(pltpu.VMEM((rows, cols), jnp.float32), pltpu.VMEM((1, cols), jnp.float32)),
        in_specs=[anywhere] * 4,
        out_specs=(vmem, vmem),
        scratch_shapes=[
            pltpu.VMEM((CHIPS * CORES, rows + EXTRA, cols), jnp.bfloat16),
            pltpu.VMEM((blocks * rows, cols), jnp.bfloat16),
            pltpu.VMEM((rows, cols), jnp.bfloat16),
            pltpu.VMEM(tile_mask.shape, jnp.int32),
            pltpu.VMEM(keep_mask.shape, jnp.int32),
            pltpu.VMEM((1, cols), jnp.int32),
            pltpu.VMEM((blocks, 1, cols), jnp.float32),
            pltpu.VMEM((CHIPS * CORES, 1, cols), jnp.float32),
            pltpu.VMEM((blocks, 1, cols), jnp.float32),
            pltpu.VMEM((EXTRA, cols), jnp.float32),
            dma((4,)),
            dma((blocks, CHUNKS)),
            dma((2,)),
            dma((CHIPS, CHUNKS)),
            dma((1,)),
            dma((CHIPS, CHUNKS)),
            dma((3,)),
            dma((3,)),
            dma((CHUNKS + 3,)),
            plain((4,)),
        ],
        compiler_params=pltpu.CompilerParams(
            collective_id=0, has_side_effects=True,
            vmem_limit_bytes=63 * 2**20 - 4 * rows * cols + 2**19,
        ),
    )(values, tile_mask, keep_mask, thr_index.reshape(1, cols))
    return (pruned * scale).astype(jnp.bfloat16)


def solution(mesh):
    return jax.shard_map(
        on_device,
        mesh=mesh,
        in_specs=(P("row", "col"), P("row", "col"), P("row", "col"), P("col")),
        out_specs=P("row", "col"),
        check_vma=False,
    )
```

```python
import functools

import jax
import jax.numpy as jnp
from jax import lax
from jax.experimental import pallas as pl
from jax.experimental.pallas import tpu as pltpu
from jax.sharding import PartitionSpec as P

TB = 128
CORES = 2
SIDE = 4
CHIPS = 8
CHUNKS = 4
LAST = 10
EXTRA = 16
LINKS = ((1, 0), (-1, 0), (0, 1), (0, -1))

ORDER = (
    ((0, 0), (1, 0), (2, 0), (3, 0), (0, 4), (2, 3), (3, 3), (2, 4), (2, 1), (3, 1), (2, 2), (3, 2), (2, 5), (2, 7), (2, 6)),
    ((1, 0), (0, 0), (3, 0), (2, 0), (1, 12), (3, 1), (2, 1), (3, 12), (3, 3), (2, 3), (3, 2), (2, 2), (3, 13), (3, 15), (3, 14)),
    ((2, 0), (3, 0), (0, 0), (1, 0), (2, 1), (0, 12), (1, 12), (0, 4), (0, 1), (1, 4), (0, 8), (0, 13), (1, 8), (0, 5), (0, 9)),
    ((3, 0), (2, 0), (1, 0), (0, 0), (3, 3), (1, 4), (0, 4), (1, 12), (1, 3), (0, 12), (1, 8), (1, 15), (1, 7), (0, 8), (1, 11)),
)
SLOTS = len(ORDER[0])
Z_ORDER = (
    tuple((c, hop) for hop in range(3) for c in (0, 1, 2, 3)) + ((0, 3), (1, 3)),
    tuple((c, hop) for hop in range(3) for c in (2, 3, 0, 1)) + ((2, 3), (3, 3)),
)
Z_SLOTS = len(Z_ORDER[0])
AHEAD = 4
POINTS = (3, 5, 7, 9, 11, 12, 13)
SUMMED = (11, 12)


def shift(place, link):
    dx, dy = LINKS[link]
    return (place // SIDE + dx) % SIDE * SIDE + (place % SIDE + dy) % SIDE


def arrivals():
    xy = {(c, shift(p, n)): s for n in range(4) for s, (c, p) in enumerate(ORDER[n])}
    z = {}
    for n, sign in ((0, 1), (1, -1)):
        for s, (c, hop) in enumerate(Z_ORDER[n]):
            z[c, sign * (hop + 1) % CHIPS] = s
    return xy, z


XY_AT, Z_AT = arrivals()
BLOCK_AT = {p: max(XY_AT[c, p] for c in range(CHUNKS)) for p in range(1, SIDE * SIDE)} | {0: 0}
Z_TAKEN = {at: at + 1 for at in range(Z_SLOTS - 2)}
NEAR_AT = [(-1, 0)] + [
    (due, due + 1) for due in (
        max(Z_TAKEN[Z_AT[c, d]] for c in range(CHUNKS) for d in (h, CHIPS - h)) for h in range(1, CHIPS // 2)
    )
] + [(SLOTS - 1.4, SLOTS - 1.2)]
NEAR_AT[-2] = (NEAR_AT[-2][0], NEAR_AT[-2][0] + 0.5)


def kernel(
    v_hbm, tile_hbm, keep_hbm, thr_hbm, acc, scale_ref,
    row_panel, col_panel, loaded, tile_ref, keep_ref, thr_ref, colsum, stats, sums, psum,
    bulk_send, xy_recv, z_recv, pair_recv,
    small_send, small_recv, load_sem, ready, hello,
):
    rows, cols = v_hbm.shape
    part = rows // CHUNKS
    order = rows * SIDE * SIDE
    me_row, me_col = lax.axis_index("row"), lax.axis_index("col")
    x, y = me_row // SIDE, me_row % SIDE
    z, core = me_col // CORES, me_col % CORES

    def xy_device(dx, dy):
        return {"row": (x + dx + SIDE) % SIDE * SIDE + (y + dy + SIDE) % SIDE}

    def z_device(dz, lane=0):
        return {"col": (z + dz + CHIPS) % CHIPS * CORES + (core if lane == 0 else 1 - core)}

    neighbours = [xy_device(*link) for link in LINKS] + [z_device(1), z_device(-1), z_device(0, 1)]
    later = [x < SIDE - 1, x == 0, y < SIDE - 1, y == 0, z < CHIPS - 1, z == 0, core == 1]
    barrier = pltpu.get_barrier_semaphore()
    earlier = 0
    for n, device in enumerate(neighbours):
        earlier = earlier + 1 - later[n].astype(jnp.int32)

        @pl.when(later[n])
        def _():
            pl.semaphore_signal(barrier, inc=1, device_id=device)

    def load(q):
        spot = pl.ds(q * part, part)
        return pltpu.make_async_copy(v_hbm.at[spot], loaded.at[spot], load_sem.at[q])

    masks = (
        pltpu.make_async_copy(tile_hbm, tile_ref, load_sem.at[CHUNKS]),
        pltpu.make_async_copy(keep_hbm, keep_ref, load_sem.at[CHUNKS + 1]),
        pltpu.make_async_copy(thr_hbm, thr_ref, load_sem.at[CHUNKS + 2]),
    )
    masks[0].start()
    for q in range(CHUNKS):
        load(q).start()
    masks[1].start()
    masks[2].start()

    def xy_copy(c, place, n):
        to = shift(place, n)
        return pltpu.make_async_remote_copy(
            src_ref=col_panel.at[pl.ds(place * rows + c * part, part)],
            dst_ref=col_panel.at[pl.ds(to * rows + c * part, part)],
            send_sem=bulk_send.at[0], recv_sem=xy_recv.at[XY_AT[c, to]],
            device_id=neighbours[n],
        )

    def z_copy(c, hop, n):
        sign = 1 - 2 * n
        spot = pl.ds(c * part, part)
        to = sign * (hop + 1) % CHIPS
        return pltpu.make_async_remote_copy(
            src_ref=row_panel.at[sign * hop % CHIPS * CORES, spot],
            dst_ref=row_panel.at[to * CORES, spot],
            send_sem=bulk_send.at[1], recv_sem=z_recv.at[Z_AT[c, to]],
            device_id=neighbours[4 + n],
        )

    def pair_copy(c, dz):
        spot = pl.ds(c * part, part)
        return pltpu.make_async_remote_copy(
            src_ref=row_panel.at[dz * CORES, spot], dst_ref=row_panel.at[dz * CORES + 1, spot],
            send_sem=bulk_send.at[1], recv_sem=pair_recv.at[min(dz, CHIPS - dz)],
            device_id=neighbours[6],
        )

    def send(n, s):
        if n < 4 and s < SLOTS:
            xy_copy(*ORDER[n][s], n).start()
        elif n == 6 and s < CHUNKS:
            pair_copy(s, 0).start()
        elif n in (4, 5) and s < Z_SLOTS:
            z_copy(*Z_ORDER[n - 4][s], n - 4).start()

    @pl.when(earlier > 0)
    def _():
        pl.semaphore_wait(barrier, earlier)

    for n, device in enumerate(neighbours):
        @pl.when(jnp.logical_not(later[n]))
        def _():
            pl.semaphore_signal(ready.at[n ^ 1 if n < 6 else n], inc=1, device_id=device)

    masks[0].wait()
    stored = tile_ref[...].astype(jnp.float32)
    for q in range(CHUNKS):
        load(q).wait()
        for lo in range(q * part, (q + 1) * part, min(part, TB)):
            for b in range(cols // TB):
                r, c = slice(lo, lo + min(part, TB)), slice(b * TB, (b + 1) * TB)
                i = lo // TB
                factor = jnp.broadcast_to(stored[i : i + 1, b : b + 1], (min(part, TB), TB))
                tile = (loaded[r, c].astype(jnp.float32) * factor).astype(jnp.bfloat16)
                row_panel[0, r, c] = tile
                col_panel[r, c] = tile

    def when_not(n, do):
        @pl.when(jnp.logical_not(later[n]))
        def _():
            do()

    for s in range(AHEAD):
        for n in range(7):
            when_not(n, lambda: send(n, s))
    for n in (6, 0, 2, 4, 1, 3, 5):
        @pl.when(later[n])
        def _():
            with jax.named_scope(f"open{n}"):
                pl.semaphore_wait(ready.at[n], 1)
            for s in range(AHEAD):
                send(n, s)

    def greet(k, over):
        for device in neighbours[4 * over : 4 + 3 * over]:
            pl.semaphore_signal(hello.at[2 * over + k % 2], inc=1, device_id=device)

    def greeted(k, over):
        pl.semaphore_wait(hello.at[2 * over + k % 2], 4 - over)

    greet(0, 0)
    greet(0, 1)

    def spread(buffer, k, count, device):
        def copy(d):
            return pltpu.make_async_remote_copy(
                src_ref=buffer.at[0], dst_ref=buffer.at[d],
                send_sem=small_send.at[0], recv_sem=small_recv.at[k], device_id=device(d),
            )

        everything = pltpu.make_async_remote_copy(
            src_ref=buffer.at[pl.ds(1, count - 1)], dst_ref=buffer.at[pl.ds(1, count - 1)],
            send_sem=small_send.at[0], recv_sem=small_recv.at[k], device_id=neighbours[6],
        )
        return [copy(d) for d in range(1, count)], everything

    def by_row(d):
        return xy_device(d // SIDE, d % SIDE)

    def by_col(d):
        return z_device(d)

    column_sums, column_sums_all = spread(colsum, 0, SIDE * SIDE, by_row)

    def sum_columns():
        total = jnp.zeros((1, cols), jnp.float32)
        for lo in range(0, rows, TB):
            block = col_panel[lo : lo + TB].astype(jnp.float32)
            total += jnp.sum(block, axis=0, keepdims=True)
        colsum[0] = total

    block_sums, block_sums_all = spread(stats, 1, CHIPS, by_col)

    def send_block_sums():
        column_sums_all.wait_recv()
        column_sums_all.wait_send()
        total = colsum[0]
        for i in range(1, SIDE * SIDE):
            total += colsum[i]
        stats[0] = total
        for copy in block_sums:
            copy.start()

    pair_sums = pltpu.make_async_remote_copy(
        src_ref=stats.at[pl.ds(0, CHIPS)], dst_ref=stats.at[pl.ds(CHIPS, CHIPS)],
        send_sem=small_send.at[0], recv_sem=small_recv.at[3], device_id=neighbours[6],
    )

    def pass_block_sums():
        block_sums_all.wait_recv()
        block_sums_all.wait_send()
        pair_sums.start()

    def take_block_sums():
        pair_sums.wait()
        line = lax.broadcasted_iota(jnp.int32, (EXTRA, cols), 0)

        @pl.loop(0, CHIPS * CORES)
        def _(i):
            rest, spot = stats[i], jnp.zeros((EXTRA, cols), jnp.float32)
            for k in range(3):
                term = rest.astype(jnp.bfloat16).astype(jnp.float32)
                rest = rest - term
                spot = jnp.where(line == k, jnp.broadcast_to(term, (EXTRA, cols)), spot)
            row_panel[i % CHIPS * CORES + i // CHIPS, rows:] = spot.astype(jnp.bfloat16)

    def inner(j):
        k = (x - j // SIDE + SIDE) % SIDE * SIDE + (y - j % SIDE + SIDE) % SIDE
        dz = (z - k // CORES + CHIPS) % CHIPS
        lane = (core + k) % CORES
        return dz, lane

    def near(dz, lane, step):
        there = None
        for side in range(CORES):
            reach = max([h for h in range(CHIPS // 2 + 1) if NEAR_AT[h][side] <= step], default=-1)
            one = (lane == side) & ((dz <= reach) | (dz >= CHIPS - reach))
            there = one if there is None else there | one
        return there

    def pick(i, values):
        found = values[0]
        for k, value in enumerate(values[1:], 1):
            found = found + (i == k).astype(jnp.int32) * (value - values[0])
        return found

    def multiply(j):
        dz, lane = inner(j)
        block = col_panel[pl.ds(pl.multiple_of(j * rows, rows), rows)]
        acc[...] += jnp.dot(
            row_panel[dz * CORES + lane, :rows], block, preferred_element_type=jnp.float32
        )

    def compute(step, before):
        fresh = [p for p in range(SIDE * SIDE) if p != LAST and before < BLOCK_AT[p] <= step]
        assert before < step
        if fresh:
            @pl.loop(0, len(fresh))
            def _(i):
                j = pick(i, fresh)

                @pl.when(near(*inner(j), step))
                def _():
                    multiply(j)

        old = [p for p in range(SIDE * SIDE) if p != LAST and BLOCK_AT[p] <= before]
        came = [
            (dz, side) for side in range(CORES) for h in range(CHIPS // 2 + 1)
            for dz in sorted({h, (CHIPS - h) % CHIPS}) if before < NEAR_AT[h][side] <= step
        ]
        if old and came:
            @pl.loop(0, len(came))
            def _(i):
                dz = pick(i, [c[0] for c in came])
                side = pick(i, [c[1] for c in came])
                k = (z - dz + CHIPS) % CHIPS * CORES + (core + side) % CORES
                j = (x - k // SIDE + SIDE) % SIDE * SIDE + (y - k % SIDE + SIDE) % SIDE
                met = j == old[0]
                for p in old[1:]:
                    met = met | (j == p)

                @pl.when(met)
                def _():
                    multiply(j)

    def add_sums(step, before):
        fresh = [p for p in range(SIDE * SIDE) if p != LAST and before < BLOCK_AT[p] <= step]

        @pl.loop(0, len(fresh))
        def _(i):
            j = pick(i, fresh)
            dz, lane = inner(j)
            block = col_panel[pl.ds(pl.multiple_of(j * rows, rows), rows)]
            psum[...] += jnp.dot(
                row_panel[dz * CORES + lane, rows:], block, preferred_element_type=jnp.float32
            )

    def await_rows(count, sem):
        spot = col_panel.at[pl.ds(0, count)]
        pltpu.make_async_remote_copy(
            src_ref=spot, dst_ref=spot, send_sem=bulk_send.at[0], recv_sem=sem, device_id=neighbours[0]
        ).wait_recv()

    def take_xy(s):
        await_rows(4 * part, xy_recv.at[s])

    def take_z(s):
        if s < Z_SLOTS:
            await_rows(2 * part, z_recv.at[s])
            for (c, dz), at in sorted(Z_AT.items()):
                if at == s:
                    pair_copy(c, dz).start()

    def take_pair(h):
        await_rows(len({h, -h % CHIPS}) * rows, pair_recv.at[h])

    before, summed = -1, -1
    for s in range(SLOTS - 1):
        if s < SLOTS - 1:
            with jax.named_scope(f"xy{s}"):
                take_xy(s)
            for n in range(4):
                send(n, s + AHEAD)
        for at in range(Z_SLOTS):
            if Z_TAKEN.get(at) == s:
                with jax.named_scope(f"z{at}"):
                    take_z(at)
        for n in (4, 5):
            if s > 0:
                send(n, s + AHEAD - 1)
        for h in range(CHIPS // 2):
            if s == NEAR_AT[h][1]:
                with jax.named_scope(f"pair{h}"):
                    take_pair(h)
        if s == Z_SLOTS - 1:
            @pl.when(z != 0)
            def _():
                take_z(s - 1)
                take_z(s)
        with jax.named_scope(f"sums{s}"):
            if s == 0:
                sum_columns()
                acc[...] = jnp.zeros((rows, cols), jnp.float32)
                psum[...] = jnp.zeros((EXTRA, cols), jnp.float32)
            if s < 3:
                greeted(s, 0)
                if s < 2:
                    greet(s + 1, 0)
            if s in (2, 4, 6):
                greeted(s // 2 - 1, 1)
                if s < 6:
                    greet(s // 2, 1)
            if s == 2:
                for copy in column_sums:
                    copy.start()
            if s == 6:
                send_block_sums()
            if s == 9:
                pass_block_sums()
            if s == 11:
                take_block_sums()
        if s in POINTS:
            with jax.named_scope(f"multiply{s}"):
                compute(s, before)
            before = s
        if s in SUMMED:
            with jax.named_scope(f"add{s}"):
                add_sums(s, summed)
            summed = s
        if s == Z_SLOTS - 2:
            with jax.named_scope("pair3"):
                take_pair(CHIPS // 2 - 1)
            with jax.named_scope("multiply3b"):
                compute(NEAR_AT[-2][1], before)
            before = NEAR_AT[-2][1]

    @pl.when(z == 0)
    def _():
        with jax.named_scope("zlast"):
            take_z(Z_SLOTS - 2)
            take_z(Z_SLOTS - 1)
    with jax.named_scope("multiplyA"):
        compute(NEAR_AT[-1][0], before)
    with jax.named_scope("addA"):
        add_sums(SLOTS - 2, summed)
    with jax.named_scope("pairlast"):
        take_pair(CHIPS // 2)
    with jax.named_scope("multiplyB"):
        compute(NEAR_AT[-1][1], NEAR_AT[-1][0])

    masks[1].wait()
    masks[2].wait()
    kept = keep_ref[...].astype(jnp.float32)
    level = 0.125 * thr_ref[...].astype(jnp.float32)
    with jax.named_scope("xy"):
        take_xy(SLOTS - 1)
    dz, lane = inner(LAST)
    slot = dz * CORES + lane
    block = col_panel[LAST * rows : (LAST + 1) * rows]
    lines = psum[...] + jnp.dot(row_panel[slot, rows:], block, preferred_element_type=jnp.float32)
    cut = level * ((lines[2:3] + lines[1:2] + lines[0:1]) / order)
    parts = [jnp.zeros((1, TB), jnp.float32) for _ in range(cols // TB)]
    for lo in range(0, rows, TB):
        term = jnp.dot(row_panel[slot, lo : lo + TB], block, preferred_element_type=jnp.float32)
        for b in range(cols // TB):
            r, c = slice(lo, lo + TB), slice(b * TB, (b + 1) * TB)
            keep = jnp.broadcast_to(kept[lo // TB : lo // TB + 1, b : b + 1], (TB, TB))
            pruned = jnp.maximum(acc[r, c] + term[:, c] - cut[:, c], 0.0) * keep
            acc[r, c] = pruned
            parts[b] += jnp.sum(pruned, axis=0, keepdims=True)
    sums[0] = jnp.concatenate(parts, axis=1)

    totals, totals_all = spread(sums, 2, SIDE * SIDE, by_row)
    for copy in totals:
        copy.start()

    for k, count in enumerate((4 * SLOTS * part, 2 * Z_SLOTS * part + CHIPS * rows)):
        spot = col_panel.at[pl.ds(0, count)]
        pltpu.make_async_remote_copy(
            src_ref=spot, dst_ref=spot, send_sem=bulk_send.at[k], recv_sem=bulk_send.at[k],
            device_id=neighbours[0],
        ).wait_send()

    with jax.named_scope("totals"):
        totals_all.wait_send()
        totals_all.wait_recv()
    total = sums[0]
    for i in range(1, SIDE * SIDE):
        total += sums[i]
    scale_ref[...] = 1.0 / jnp.maximum(total / order, 0.1)


def on_device(values, tile_mask, keep_mask, thr_index):
    rows, cols = values.shape
    dma, plain = pltpu.SemaphoreType.DMA, pltpu.SemaphoreType.REGULAR
    vmem, anywhere = pl.BlockSpec(memory_space=pltpu.VMEM), pl.BlockSpec(memory_space=pl.ANY)
    blocks = SIDE * SIDE
    pruned, scale = pl.pallas_call(
        kernel,
        out_shape=(pltpu.VMEM((rows, cols), jnp.float32), pltpu.VMEM((1, cols), jnp.float32)),
        in_specs=[anywhere] * 4,
        out_specs=(vmem, vmem),
        scratch_shapes=[
            pltpu.VMEM((CHIPS * CORES, rows + EXTRA, cols), jnp.bfloat16),
            pltpu.VMEM((blocks * rows, cols), jnp.bfloat16),
            pltpu.VMEM((rows, cols), jnp.bfloat16),
            pltpu.VMEM(tile_mask.shape, jnp.int32),
            pltpu.VMEM(keep_mask.shape, jnp.int32),
            pltpu.VMEM((1, cols), jnp.int32),
            pltpu.VMEM((blocks, 1, cols), jnp.float32),
            pltpu.VMEM((CHIPS * CORES, 1, cols), jnp.float32),
            pltpu.VMEM((blocks, 1, cols), jnp.float32),
            pltpu.VMEM((EXTRA, cols), jnp.float32),
            dma((2,)),
            dma((SLOTS,)),
            dma((Z_SLOTS,)),
            dma((CHIPS // 2 + 1,)),
            dma((1,)),
            dma((4,)),
            dma((CHUNKS + 3,)),
            plain((7,)),
            plain((4,)),
        ],
        compiler_params=pltpu.CompilerParams(
            collective_id=0, has_side_effects=True,
            vmem_limit_bytes=63 * 2**20 - 4 * rows * cols + 2**19,
        ),
    )(values, tile_mask, keep_mask, thr_index.reshape(1, cols))
    return (pruned * scale).astype(jnp.bfloat16)


def solution(mesh):
    return jax.shard_map(
        on_device,
        mesh=mesh,
        in_specs=(P("row", "col"), P("row", "col"), P("row", "col"), P("col")),
        out_specs=P("row", "col"),
        check_vma=False,
    )
```

```python
import functools

import jax
import jax.numpy as jnp
from jax import lax
from jax.experimental import pallas as pl
from jax.experimental.pallas import tpu as pltpu
from jax.sharding import PartitionSpec as P

TB = 128
CORES = 2
SIDE = 4
CHIPS = 8
CHUNKS = 4
LAST = 10
EXTRA = 16
LINKS = ((1, 0), (-1, 0), (0, 1), (0, -1))

ORDER = (
    ((0, 0), (1, 0), (2, 0), (3, 0), (0, 4), (2, 3), (3, 3), (2, 4), (2, 1), (3, 1), (2, 2), (3, 2), (2, 5), (2, 7), (2, 6)),
    ((1, 0), (0, 0), (3, 0), (2, 0), (1, 12), (3, 1), (2, 1), (3, 12), (3, 3), (2, 3), (3, 2), (2, 2), (3, 13), (3, 15), (3, 14)),
    ((2, 0), (3, 0), (0, 0), (1, 0), (2, 1), (0, 12), (1, 12), (0, 4), (0, 1), (1, 4), (0, 8), (0, 13), (1, 8), (0, 5), (0, 9)),
    ((3, 0), (2, 0), (1, 0), (0, 0), (3, 3), (1, 4), (0, 4), (1, 12), (1, 3), (0, 12), (1, 8), (1, 15), (1, 7), (0, 8), (1, 11)),
)
SLOTS = len(ORDER[0])
Z_ORDER = (
    tuple((c, hop) for hop in range(3) for c in (1, 0, 2, 3)) + ((1, 3), (0, 3)),
    tuple((c, hop) for hop in range(3) for c in (2, 3, 0, 1)) + ((2, 3), (3, 3)),
)
DETOUR = (0, 3)
Z_SLOTS = len(Z_ORDER[0])
AHEAD = 4
POINTS = (3, 5, 7, 9, 11, 12, 13)
SUMMED = 10


def shift(place, link):
    dx, dy = LINKS[link]
    return (place // SIDE + dx) % SIDE * SIDE + (place % SIDE + dy) % SIDE


def arrivals():
    xy = {(c, shift(p, n)): s for n in range(4) for s, (c, p) in enumerate(ORDER[n])}
    z = {}
    for n, sign in ((0, 1), (1, -1)):
        for s, (c, hop) in enumerate(Z_ORDER[n]):
            z[c, sign * (hop + 1) % CHIPS] = s
    return xy, z


XY_AT, Z_AT = arrivals()
BLOCK_AT = {p: max(XY_AT[c, p] for c in range(CHUNKS)) for p in range(1, SIDE * SIDE)} | {0: 0}
Z_LAG = 10
NEAR_AT = [(-1, 0), (4, 5), (8, 9), (11.5, 12.5), (13.6, 13.8)]


def kernel(
    v_hbm, tile_hbm, keep_hbm, thr_hbm, acc, scale_ref,
    row_panel, col_panel, loaded, tile_ref, keep_ref, thr_ref, colsum, stats, sums, psum,
    bulk_send, xy_recv, z_recv, pair_recv,
    detour_send, small_send, small_recv, load_sem, ready, hello,
):
    rows, cols = v_hbm.shape
    part = rows // CHUNKS
    order = rows * SIDE * SIDE
    me_row, me_col = lax.axis_index("row"), lax.axis_index("col")
    x, y = me_row // SIDE, me_row % SIDE
    z, core = me_col // CORES, me_col % CORES

    def xy_device(dx, dy):
        return {"row": (x + dx + SIDE) % SIDE * SIDE + (y + dy + SIDE) % SIDE}

    def z_device(dz, lane=0):
        return {"col": (z + dz + CHIPS) % CHIPS * CORES + (core if lane == 0 else 1 - core)}

    neighbours = [xy_device(*link) for link in LINKS] + [z_device(1), z_device(-1), z_device(0, 1)]
    later = [x < SIDE - 1, x == 0, y < SIDE - 1, y == 0, z < CHIPS - 1, z == 0, core == 1]
    barrier = pltpu.get_barrier_semaphore()
    earlier = 0
    for n, device in enumerate(neighbours):
        earlier = earlier + 1 - later[n].astype(jnp.int32)

        @pl.when(later[n])
        def _():
            pl.semaphore_signal(barrier, inc=1, device_id=device)

    def load(q):
        spot = pl.ds(q * part, part)
        return pltpu.make_async_copy(v_hbm.at[spot], loaded.at[spot], load_sem.at[q])

    masks = (
        pltpu.make_async_copy(tile_hbm, tile_ref, load_sem.at[CHUNKS]),
        pltpu.make_async_copy(keep_hbm, keep_ref, load_sem.at[CHUNKS + 1]),
        pltpu.make_async_copy(thr_hbm, thr_ref, load_sem.at[CHUNKS + 2]),
    )
    masks[0].start()
    for q in range(CHUNKS):
        load(q).start()
    masks[1].start()
    masks[2].start()

    def xy_copy(c, place, n):
        to = shift(place, n)
        return pltpu.make_async_remote_copy(
            src_ref=col_panel.at[pl.ds(place * rows + c * part, part)],
            dst_ref=col_panel.at[pl.ds(to * rows + c * part, part)],
            send_sem=bulk_send.at[0], recv_sem=xy_recv.at[XY_AT[c, to]],
            device_id=neighbours[n],
        )

    def z_copy(c, hop, n, sent=None):
        sign = 1 - 2 * n
        spot = pl.ds(c * part, part)
        to = sign * (hop + 1) % CHIPS
        return pltpu.make_async_remote_copy(
            src_ref=row_panel.at[sign * hop % CHIPS * CORES, spot],
            dst_ref=row_panel.at[to * CORES, spot],
            send_sem=bulk_send.at[1] if sent is None else sent, recv_sem=z_recv.at[Z_AT[c, to]],
            device_id=neighbours[4 + n],
        )

    def pair_copy(c, dz):
        spot = pl.ds(c * part, part)
        return pltpu.make_async_remote_copy(
            src_ref=row_panel.at[dz * CORES, spot], dst_ref=row_panel.at[dz * CORES + 1, spot],
            send_sem=bulk_send.at[1], recv_sem=pair_recv.at[min(dz, CHIPS - dz)],
            device_id=neighbours[6],
        )

    def send(n, s):
        if n < 4 and s < SLOTS:
            xy_copy(*ORDER[n][s], n).start()
        elif n == 6 and s < CHUNKS:
            pair_copy(s, 0).start()
        elif n in (4, 5) and s < Z_SLOTS:
            if n == 4 and Z_ORDER[0][s] == DETOUR:
                @pl.when(z != CHIPS - 1)
                def _():
                    z_copy(*DETOUR, 0, detour_send.at[0]).start()
            else:
                z_copy(*Z_ORDER[n - 4][s], n - 4).start()

    @pl.when(earlier > 0)
    def _():
        pl.semaphore_wait(barrier, earlier)

    for n, device in enumerate(neighbours):
        @pl.when(jnp.logical_not(later[n]))
        def _():
            pl.semaphore_signal(ready.at[n ^ 1 if n < 6 else n], inc=1, device_id=device)

    masks[0].wait()
    stored = tile_ref[...].astype(jnp.float32)
    for q in range(CHUNKS):
        load(q).wait()
        for lo in range(q * part, (q + 1) * part, min(part, TB)):
            for b in range(cols // TB):
                r, c = slice(lo, lo + min(part, TB)), slice(b * TB, (b + 1) * TB)
                i = lo // TB
                factor = jnp.broadcast_to(stored[i : i + 1, b : b + 1], (min(part, TB), TB))
                tile = (loaded[r, c].astype(jnp.float32) * factor).astype(jnp.bfloat16)
                row_panel[0, r, c] = tile
                col_panel[r, c] = tile

    def when_not(n, do):
        @pl.when(jnp.logical_not(later[n]))
        def _():
            do()

    for s in range(AHEAD - 1):
        for n in range(6):
            when_not(n, lambda: send(n, s))
    for n in (6, 0, 2, 4, 1, 3, 5):
        if n == 6:
            when_not(n, lambda: [send(n, s) for s in range(CHUNKS)])

        @pl.when(later[n])
        def _():
            with jax.named_scope(f"open{n}"):
                pl.semaphore_wait(ready.at[n], 1)
            for s in range(CHUNKS if n == 6 else AHEAD - 1):
                send(n, s)

    def greet(k, over):
        for device in neighbours[4 * over : 4 + 3 * over]:
            pl.semaphore_signal(hello.at[2 * over + k % 2], inc=1, device_id=device)

    def greeted(k, over):
        pl.semaphore_wait(hello.at[2 * over + k % 2], 4 - over)

    greet(0, 0)
    greet(0, 1)

    def spread(buffer, k, count, device):
        def copy(d):
            return pltpu.make_async_remote_copy(
                src_ref=buffer.at[0], dst_ref=buffer.at[d],
                send_sem=small_send.at[0], recv_sem=small_recv.at[k], device_id=device(d),
            )

        everything = pltpu.make_async_remote_copy(
            src_ref=buffer.at[pl.ds(1, count - 1)], dst_ref=buffer.at[pl.ds(1, count - 1)],
            send_sem=small_send.at[0], recv_sem=small_recv.at[k], device_id=neighbours[6],
        )
        return [copy(d) for d in range(1, count)], everything

    def by_row(d):
        return xy_device(d // SIDE, d % SIDE)

    def by_col(d):
        return z_device(d)

    column_sums, column_sums_all = spread(colsum, 0, SIDE * SIDE, by_row)

    total = jnp.zeros((1, cols), jnp.float32)
    for lo in range(0, rows, TB):
        block = col_panel[lo : lo + TB].astype(jnp.float32)
        total += jnp.sum(block, axis=0, keepdims=True)
    colsum[0] = total
    acc[...] = jnp.zeros((rows, cols), jnp.float32)
    psum[...] = jnp.zeros((EXTRA, cols), jnp.float32)
    with jax.named_scope("greet"):
        for k in range(3):
            greeted(k, 0)
            if k < 2:
                greet(k + 1, 0)
    for copy in column_sums:
        copy.start()
    for n in range(6):
        send(n, AHEAD - 1)

    block_sums, block_sums_all = spread(stats, 1, CHIPS, by_col)

    def send_block_sums():
        column_sums_all.wait_recv()
        column_sums_all.wait_send()
        total = colsum[0]
        for i in range(1, SIDE * SIDE):
            total += colsum[i]
        stats[0] = total
        for copy in block_sums:
            copy.start()

    pair_sums = pltpu.make_async_remote_copy(
        src_ref=stats.at[pl.ds(0, CHIPS)], dst_ref=stats.at[pl.ds(CHIPS, CHIPS)],
        send_sem=small_send.at[0], recv_sem=small_recv.at[3], device_id=neighbours[6],
    )

    def pass_block_sums():
        block_sums_all.wait_recv()
        block_sums_all.wait_send()
        pair_sums.start()

    def take_block_sums():
        pair_sums.wait()
        line = lax.broadcasted_iota(jnp.int32, (EXTRA, cols), 0)

        @pl.loop(0, CHIPS * CORES)
        def _(i):
            rest, spot = stats[i], jnp.zeros((EXTRA, cols), jnp.float32)
            for k in range(3):
                term = rest.astype(jnp.bfloat16).astype(jnp.float32)
                rest = rest - term
                spot = jnp.where(line == k, jnp.broadcast_to(term, (EXTRA, cols)), spot)
            row_panel[i % CHIPS * CORES + i // CHIPS, rows:] = spot.astype(jnp.bfloat16)

    def inner(j):
        k = (x - j // SIDE + SIDE) % SIDE * SIDE + (y - j % SIDE + SIDE) % SIDE
        dz = (z - k // CORES + CHIPS) % CHIPS
        lane = (core + k) % CORES
        return dz, lane

    def near(dz, lane, step):
        there = None
        for side in range(CORES):
            reach = max([h for h in range(CHIPS // 2 + 1) if NEAR_AT[h][side] <= step], default=-1)
            one = (lane == side) & ((dz <= reach) | (dz >= CHIPS - reach))
            there = one if there is None else there | one
        return there

    def pick(i, values):
        found = values[0]
        for k, value in enumerate(values[1:], 1):
            found = found + (i == k).astype(jnp.int32) * (value - values[0])
        return found

    def multiply(j, summed):
        dz, lane = inner(j)
        block = col_panel[pl.ds(pl.multiple_of(j * rows, rows), rows)]
        if summed:
            term = jnp.dot(row_panel[dz * CORES + lane], block, preferred_element_type=jnp.float32)
            acc[...] += term[:rows]
            psum[...] += term[rows:]
        else:
            acc[...] += jnp.dot(
                row_panel[dz * CORES + lane, :rows], block, preferred_element_type=jnp.float32
            )

    def compute(step, before):
        fresh = [p for p in range(SIDE * SIDE) if p != LAST and before < BLOCK_AT[p] <= step]
        assert before < step
        if fresh:
            @pl.loop(0, len(fresh))
            def _(i):
                j = pick(i, fresh)

                @pl.when(near(*inner(j), step))
                def _():
                    multiply(j, step > SUMMED)

        old = [p for p in range(SIDE * SIDE) if p != LAST and BLOCK_AT[p] <= before]
        came = [
            (dz, side) for side in range(CORES) for h in range(CHIPS // 2 + 1)
            for dz in sorted({h, (CHIPS - h) % CHIPS}) if before < NEAR_AT[h][side] <= step
        ]
        if old and came:
            @pl.loop(0, len(came))
            def _(i):
                dz = pick(i, [c[0] for c in came])
                side = pick(i, [c[1] for c in came])
                k = (z - dz + CHIPS) % CHIPS * CORES + (core + side) % CORES
                j = (x - k // SIDE + SIDE) % SIDE * SIDE + (y - k % SIDE + SIDE) % SIDE
                met = j == old[0]
                for p in old[1:]:
                    met = met | (j == p)

                @pl.when(met)
                def _():
                    multiply(j, step > SUMMED)

    def add_sums(step):
        fresh = [p for p in range(SIDE * SIDE) if BLOCK_AT[p] <= step]

        @pl.loop(0, len(fresh))
        def _(i):
            j = pick(i, fresh)
            dz, lane = inner(j)

            @pl.when(near(dz, lane, step))
            def _():
                block = col_panel[pl.ds(pl.multiple_of(j * rows, rows), rows)]
                psum[...] += jnp.dot(
                    row_panel[dz * CORES + lane, rows:], block, preferred_element_type=jnp.float32
                )

    def await_rows(count, sem):
        spot = col_panel.at[pl.ds(0, count)]
        pltpu.make_async_remote_copy(
            src_ref=spot, dst_ref=spot, send_sem=bulk_send.at[0], recv_sem=sem, device_id=neighbours[0]
        ).wait_recv()

    def take_xy(s):
        await_rows(4 * part, xy_recv.at[s])

    def take_z(s):
        if s < Z_SLOTS:
            await_rows(2 * part, z_recv.at[s])
            for (c, dz), at in sorted(Z_AT.items()):
                if at == s:
                    pair_copy(c, dz).start()

    def take_pair(h):
        await_rows(len({h, -h % CHIPS}) * rows, pair_recv.at[h])

    before = -1
    for s in range(SLOTS - 1):
        if s < SLOTS - 1:
            with jax.named_scope(f"xy{s}"):
                take_xy(s)
            for n in range(4):
                send(n, s + AHEAD)
        if 0 < s <= Z_LAG:
            with jax.named_scope(f"z{s - 1}"):
                take_z(s - 1)
        for n in (4, 5):
            if s > 0:
                send(n, s + AHEAD - 1)
        for h in range(CHIPS // 2):
            if s == NEAR_AT[h][1]:
                with jax.named_scope(f"pair{h}"):
                    take_pair(h)
        if s == Z_SLOTS - 1:
            with jax.named_scope(f"z{s}"):
                take_z(s)
        with jax.named_scope(f"sums{s}"):
            if s < 3:
                greeted(s, 1)
                if s < 2:
                    greet(s + 1, 1)
            if s == 3:
                send_block_sums()
            if s == SUMMED - 1:
                pass_block_sums()
            if s == SUMMED:
                take_block_sums()
                add_sums(before)
        if s in POINTS:
            with jax.named_scope(f"multiply{s}"):
                compute(s, before)
            before = s
        if s == Z_SLOTS - 2:
            with jax.named_scope("pair3"):
                take_pair(CHIPS // 2 - 1)
            with jax.named_scope("multiply3b"):
                compute(NEAR_AT[-2][1], before)
            before = NEAR_AT[-2][1]
        if Z_LAG <= s < Z_SLOTS - 1:
            with jax.named_scope(f"z{s}"):
                take_z(s)
            if s == Z_AT[DETOUR[0], CHIPS - DETOUR[1]]:
                @pl.when(z == 1)
                def _():
                    z_copy(*DETOUR, 1, detour_send.at[1]).start()

    with jax.named_scope("multiplyA"):
        compute(NEAR_AT[-1][0], before)
    with jax.named_scope("pairlast"):
        take_pair(CHIPS // 2)
    with jax.named_scope("multiplyB"):
        compute(NEAR_AT[-1][1], NEAR_AT[-1][0])

    masks[1].wait()
    masks[2].wait()
    kept = keep_ref[...].astype(jnp.float32)
    level = 0.125 * thr_ref[...].astype(jnp.float32)
    with jax.named_scope("xy"):
        take_xy(SLOTS - 1)
    dz, lane = inner(LAST)
    slot = dz * CORES + lane
    block = col_panel[LAST * rows : (LAST + 1) * rows]
    lines = psum[...] + jnp.dot(row_panel[slot, rows:], block, preferred_element_type=jnp.float32)
    cut = level * ((lines[2:3] + lines[1:2] + lines[0:1]) / order)
    parts = [jnp.zeros((1, TB), jnp.float32) for _ in range(cols // TB)]
    for lo in range(0, rows, TB):
        term = jnp.dot(row_panel[slot, lo : lo + TB], block, preferred_element_type=jnp.float32)
        for b in range(cols // TB):
            r, c = slice(lo, lo + TB), slice(b * TB, (b + 1) * TB)
            keep = jnp.broadcast_to(kept[lo // TB : lo // TB + 1, b : b + 1], (TB, TB))
            pruned = jnp.maximum(acc[r, c] + term[:, c] - cut[:, c], 0.0) * keep
            acc[r, c] = pruned
            parts[b] += jnp.sum(pruned, axis=0, keepdims=True)
    sums[0] = jnp.concatenate(parts, axis=1)

    totals, totals_all = spread(sums, 2, SIDE * SIDE, by_row)
    for copy in totals:
        copy.start()

    for k, count in enumerate((4 * SLOTS * part, (2 * Z_SLOTS - 1) * part + CHIPS * rows)):
        spot = col_panel.at[pl.ds(0, count)]
        pltpu.make_async_remote_copy(
            src_ref=spot, dst_ref=spot, send_sem=bulk_send.at[k], recv_sem=bulk_send.at[k],
            device_id=neighbours[0],
        ).wait_send()

    for n, sends in ((0, z != CHIPS - 1), (1, z == 1)):
        @pl.when(sends)
        def _():
            z_copy(*DETOUR, n, detour_send.at[n]).wait_send()

    with jax.named_scope("totals"):
        totals_all.wait_send()
        totals_all.wait_recv()
    total = sums[0]
    for i in range(1, SIDE * SIDE):
        total += sums[i]
    scale_ref[...] = 1.0 / jnp.maximum(total / order, 0.1)


def on_device(values, tile_mask, keep_mask, thr_index):
    rows, cols = values.shape
    dma, plain = pltpu.SemaphoreType.DMA, pltpu.SemaphoreType.REGULAR
    vmem, anywhere = pl.BlockSpec(memory_space=pltpu.VMEM), pl.BlockSpec(memory_space=pl.ANY)
    blocks = SIDE * SIDE
    pruned, scale = pl.pallas_call(
        kernel,
        out_shape=(pltpu.VMEM((rows, cols), jnp.float32), pltpu.VMEM((1, cols), jnp.float32)),
        in_specs=[anywhere] * 4,
        out_specs=(vmem, vmem),
        scratch_shapes=[
            pltpu.VMEM((CHIPS * CORES, rows + EXTRA, cols), jnp.bfloat16),
            pltpu.VMEM((blocks * rows, cols), jnp.bfloat16),
            pltpu.VMEM((rows, cols), jnp.bfloat16),
            pltpu.VMEM(tile_mask.shape, jnp.int32),
            pltpu.VMEM(keep_mask.shape, jnp.int32),
            pltpu.VMEM((1, cols), jnp.int32),
            pltpu.VMEM((blocks, 1, cols), jnp.float32),
            pltpu.VMEM((CHIPS * CORES, 1, cols), jnp.float32),
            pltpu.VMEM((blocks, 1, cols), jnp.float32),
            pltpu.VMEM((EXTRA, cols), jnp.float32),
            dma((2,)),
            dma((SLOTS,)),
            dma((Z_SLOTS,)),
            dma((CHIPS // 2 + 1,)),
            dma((2,)),
            dma((1,)),
            dma((4,)),
            dma((CHUNKS + 3,)),
            plain((7,)),
            plain((4,)),
        ],
        compiler_params=pltpu.CompilerParams(
            collective_id=0, has_side_effects=True,
            vmem_limit_bytes=63 * 2**20 - 4 * rows * cols + 2**19,
        ),
    )(values, tile_mask, keep_mask, thr_index.reshape(1, cols))
    return (pruned * scale).astype(jnp.bfloat16)


def solution(mesh):
    return jax.shard_map(
        on_device,
        mesh=mesh,
        in_specs=(P("row", "col"), P("row", "col"), P("row", "col"), P("col")),
        out_specs=P("row", "col"),
        check_vma=False,
    )
```

```python
import functools

import jax
import jax.numpy as jnp
from jax import lax
from jax.experimental import pallas as pl
from jax.experimental.pallas import tpu as pltpu
from jax.sharding import PartitionSpec as P

TB = 128
CORES = 2
SIDE = 4
CHIPS = 8
CHUNKS = 4
LAST = 10
EXTRA = 16
LINKS = ((1, 0), (-1, 0), (0, 1), (0, -1))

ORDER = (
    ((0, 0), (1, 0), (2, 0), (3, 0), (0, 4), (2, 3), (3, 3), (2, 4), (2, 1), (3, 1), (2, 2), (3, 2), (2, 5), (2, 7), (2, 6)),
    ((1, 0), (0, 0), (3, 0), (2, 0), (1, 12), (3, 1), (2, 1), (3, 12), (3, 3), (2, 3), (3, 2), (2, 2), (3, 13), (3, 15), (3, 14)),
    ((2, 0), (3, 0), (0, 0), (1, 0), (2, 1), (0, 12), (1, 12), (0, 4), (0, 1), (1, 4), (0, 8), (0, 13), (1, 8), (0, 5), (0, 9)),
    ((3, 0), (2, 0), (1, 0), (0, 0), (3, 3), (1, 4), (0, 4), (1, 12), (1, 3), (0, 12), (1, 8), (1, 15), (1, 7), (0, 8), (1, 11)),
)
SLOTS = len(ORDER[0])
Z_ORDER = (
    tuple((c, hop) for hop in range(3) for c in (1, 0, 2, 3)) + ((1, 3), (0, 3)),
    tuple((c, hop) for hop in range(3) for c in (2, 3, 0, 1)) + ((2, 3), (3, 3)),
)
DETOUR = (0, 3)
Z_SLOTS = len(Z_ORDER[0])
AHEAD = 4
POINTS = (3, 5, 7, 9, 11, 12, 13)
SUMMED = 10


def shift(place, link):
    dx, dy = LINKS[link]
    return (place // SIDE + dx) % SIDE * SIDE + (place % SIDE + dy) % SIDE


def arrivals():
    xy = {(c, shift(p, n)): s for n in range(4) for s, (c, p) in enumerate(ORDER[n])}
    z = {}
    for n, sign in ((0, 1), (1, -1)):
        for s, (c, hop) in enumerate(Z_ORDER[n]):
            z[c, sign * (hop + 1) % CHIPS] = s
    return xy, z


XY_AT, Z_AT = arrivals()
BLOCK_AT = {p: max(XY_AT[c, p] for c in range(CHUNKS)) for p in range(1, SIDE * SIDE)} | {0: 0}
Z_LAG = 10
NEAR_AT = [(-1, 0), (4, 5), (8, 9), (11.5, 12.5), (13.6, 13.8)]


def kernel(
    v_hbm, tile_hbm, keep_hbm, thr_hbm, acc, scale_ref,
    row_panel, col_panel, loaded, tile_ref, keep_ref, thr_ref, colsum, stats, sums, psum,
    bulk_send, xy_recv, z_recv, pair_recv,
    detour_send, small_send, small_recv, load_sem, ready, hello,
):
    rows, cols = v_hbm.shape
    part = rows // CHUNKS
    order = rows * SIDE * SIDE
    me_row, me_col = lax.axis_index("row"), lax.axis_index("col")
    x, y = me_row // SIDE, me_row % SIDE
    z, core = me_col // CORES, me_col % CORES

    def xy_device(dx, dy):
        return {"row": (x + dx + SIDE) % SIDE * SIDE + (y + dy + SIDE) % SIDE}

    def z_device(dz, lane=0):
        return {"col": (z + dz + CHIPS) % CHIPS * CORES + (core if lane == 0 else 1 - core)}

    neighbours = [xy_device(*link) for link in LINKS] + [z_device(1), z_device(-1), z_device(0, 1)]
    later = [x < SIDE - 1, x == 0, y < SIDE - 1, y == 0, z < CHIPS - 1, z == 0, core == 1]
    barrier = pltpu.get_barrier_semaphore()
    earlier = 0
    for n, device in enumerate(neighbours):
        earlier = earlier + 1 - later[n].astype(jnp.int32)

        @pl.when(later[n])
        def _():
            pl.semaphore_signal(barrier, inc=1, device_id=device)

    def load(q):
        spot = pl.ds(q * part, part)
        return pltpu.make_async_copy(v_hbm.at[spot], loaded.at[spot], load_sem.at[q])

    masks = (
        pltpu.make_async_copy(tile_hbm, tile_ref, load_sem.at[CHUNKS]),
        pltpu.make_async_copy(keep_hbm, keep_ref, load_sem.at[CHUNKS + 1]),
        pltpu.make_async_copy(thr_hbm, thr_ref, load_sem.at[CHUNKS + 2]),
    )
    masks[0].start()
    for q in range(CHUNKS):
        load(q).start()
    masks[1].start()
    masks[2].start()

    def xy_copy(c, place, n):
        to = shift(place, n)
        return pltpu.make_async_remote_copy(
            src_ref=col_panel.at[pl.ds(place * rows + c * part, part)],
            dst_ref=col_panel.at[pl.ds(to * rows + c * part, part)],
            send_sem=bulk_send.at[0], recv_sem=xy_recv.at[XY_AT[c, to]],
            device_id=neighbours[n],
        )

    def z_copy(c, hop, n, sent=None, lo=0, count=part):
        sign = 1 - 2 * n
        spot = pl.ds(c * part + lo, count)
        to = sign * (hop + 1) % CHIPS
        return pltpu.make_async_remote_copy(
            src_ref=row_panel.at[sign * hop % CHIPS * CORES, spot],
            dst_ref=row_panel.at[to * CORES, spot],
            send_sem=bulk_send.at[1] if sent is None else sent, recv_sem=z_recv.at[Z_AT[c, to]],
            device_id=neighbours[4 + n],
        )

    def pair_copy(c, dz):
        spot = pl.ds(c * part, part)
        return pltpu.make_async_remote_copy(
            src_ref=row_panel.at[dz * CORES, spot], dst_ref=row_panel.at[dz * CORES + 1, spot],
            send_sem=bulk_send.at[1], recv_sem=pair_recv.at[min(dz, CHIPS - dz)],
            device_id=neighbours[6],
        )

    def send(n, s):
        if n < 4 and s < SLOTS:
            xy_copy(*ORDER[n][s], n).start()
        elif n == 6 and s < CHUNKS:
            pair_copy(s, 0).start()
        elif n in (4, 5) and s < Z_SLOTS:
            if n == 4 and Z_ORDER[0][s] == DETOUR:
                @pl.when(z != CHIPS - 1)
                def _():
                    z_copy(*DETOUR, 0, detour_send.at[0]).start()

                @pl.when(z == CHIPS - 1)
                def _():
                    z_copy(*DETOUR, 0, detour_send.at[0], 0, part // 2).start()
            else:
                z_copy(*Z_ORDER[n - 4][s], n - 4).start()

    @pl.when(earlier > 0)
    def _():
        pl.semaphore_wait(barrier, earlier)

    for n, device in enumerate(neighbours):
        @pl.when(jnp.logical_not(later[n]))
        def _():
            pl.semaphore_signal(ready.at[n ^ 1 if n < 6 else n], inc=1, device_id=device)

    masks[0].wait()
    stored = tile_ref[...].astype(jnp.float32)
    for q in range(CHUNKS):
        load(q).wait()
        for lo in range(q * part, (q + 1) * part, TB):
            for b in range(cols // TB):
                r, c = slice(lo, lo + TB), slice(b * TB, (b + 1) * TB)
                i = lo // TB
                factor = jnp.broadcast_to(stored[i : i + 1, b : b + 1], (EXTRA, TB)).astype(jnp.bfloat16)
                tile = loaded[r, c] * jnp.concatenate([factor] * (TB // EXTRA), axis=0)
                row_panel[0, r, c] = tile
                col_panel[r, c] = tile

    def when_not(n, do):
        @pl.when(jnp.logical_not(later[n]))
        def _():
            do()

    for s in range(AHEAD - 1):
        for n in range(6):
            when_not(n, lambda: send(n, s))
    for n in (6, 0, 2, 4, 1, 3, 5):
        if n == 6:
            when_not(n, lambda: [send(n, s) for s in range(CHUNKS)])

        @pl.when(later[n])
        def _():
            with jax.named_scope(f"open{n}"):
                pl.semaphore_wait(ready.at[n], 1)
            for s in range(CHUNKS if n == 6 else AHEAD - 1):
                send(n, s)

    def greet(k, over):
        for device in neighbours[4 * over : 4 + 3 * over]:
            pl.semaphore_signal(hello.at[2 * over + k % 2], inc=1, device_id=device)

    def greeted(k, over):
        pl.semaphore_wait(hello.at[2 * over + k % 2], 4 - over)

    greet(0, 0)
    greet(0, 1)

    def spread(buffer, k, count, device):
        def copy(d):
            return pltpu.make_async_remote_copy(
                src_ref=buffer.at[0], dst_ref=buffer.at[d],
                send_sem=small_send.at[0], recv_sem=small_recv.at[k], device_id=device(d),
            )

        everything = pltpu.make_async_remote_copy(
            src_ref=buffer.at[pl.ds(1, count - 1)], dst_ref=buffer.at[pl.ds(1, count - 1)],
            send_sem=small_send.at[0], recv_sem=small_recv.at[k], device_id=neighbours[6],
        )
        return [copy(d) for d in range(1, count)], everything

    def by_row(d):
        return xy_device(d // SIDE, d % SIDE)

    def by_col(d):
        return z_device(d)

    column_sums, column_sums_all = spread(colsum, 0, SIDE * SIDE, by_row)

    total = jnp.zeros((1, cols), jnp.float32)
    for lo in range(0, rows, TB):
        block = col_panel[lo : lo + TB].astype(jnp.float32)
        total += jnp.sum(block, axis=0, keepdims=True)
    colsum[0] = total
    acc[...] = jnp.zeros((rows, cols), jnp.float32)
    psum[...] = jnp.zeros((EXTRA, cols), jnp.float32)
    with jax.named_scope("greet"):
        for k in range(3):
            greeted(k, 0)
            if k < 2:
                greet(k + 1, 0)
    for copy in column_sums:
        copy.start()
    for n in range(6):
        send(n, AHEAD - 1)

    block_sums, block_sums_all = spread(stats, 1, CHIPS, by_col)

    def send_block_sums():
        column_sums_all.wait_recv()
        column_sums_all.wait_send()
        total = colsum[0]
        for i in range(1, SIDE * SIDE):
            total += colsum[i]
        stats[0] = total
        for copy in block_sums:
            copy.start()

    pair_sums = pltpu.make_async_remote_copy(
        src_ref=stats.at[pl.ds(0, CHIPS)], dst_ref=stats.at[pl.ds(CHIPS, CHIPS)],
        send_sem=small_send.at[0], recv_sem=small_recv.at[3], device_id=neighbours[6],
    )

    def pass_block_sums():
        block_sums_all.wait_recv()
        block_sums_all.wait_send()
        pair_sums.start()

    def take_block_sums():
        pair_sums.wait()
        line = lax.broadcasted_iota(jnp.int32, (EXTRA, cols), 0)

        @pl.loop(0, CHIPS * CORES)
        def _(i):
            rest, spot = stats[i], jnp.zeros((EXTRA, cols), jnp.float32)
            for k in range(3):
                term = rest.astype(jnp.bfloat16).astype(jnp.float32)
                rest = rest - term
                spot = jnp.where(line == k, jnp.broadcast_to(term, (EXTRA, cols)), spot)
            row_panel[i % CHIPS * CORES + i // CHIPS, rows:] = spot.astype(jnp.bfloat16)

    def inner(j):
        k = (x - j // SIDE + SIDE) % SIDE * SIDE + (y - j % SIDE + SIDE) % SIDE
        dz = (z - k // CORES + CHIPS) % CHIPS
        lane = (core + k) % CORES
        return dz, lane

    def near(dz, lane, step):
        there = None
        for side in range(CORES):
            reach = max([h for h in range(CHIPS // 2 + 1) if NEAR_AT[h][side] <= step], default=-1)
            one = (lane == side) & ((dz <= reach) | (dz >= CHIPS - reach))
            there = one if there is None else there | one
        return there

    def pick(i, values):
        found = values[0]
        for k, value in enumerate(values[1:], 1):
            found = found + (i == k).astype(jnp.int32) * (value - values[0])
        return found

    def met(of):
        dz, side = of
        k = (z - dz + CHIPS) % CHIPS * CORES + (core + side) % CORES
        return (x - k // SIDE + SIDE) % SIDE * SIDE + (y - k % SIDE + SIDE) % SIDE

    def multiply(j, summed):
        dz, lane = inner(j)
        block = col_panel[pl.ds(pl.multiple_of(j * rows, rows), rows)]
        if summed:
            term = jnp.dot(row_panel[dz * CORES + lane], block, preferred_element_type=jnp.float32)
            acc[...] += term[:rows]
            psum[...] += term[rows:]
        else:
            acc[...] += jnp.dot(
                row_panel[dz * CORES + lane, :rows], block, preferred_element_type=jnp.float32
            )

    def compute(step, before):
        fresh = [p for p in range(SIDE * SIDE) if p != LAST and before < BLOCK_AT[p] <= step]
        assert before < step
        if fresh:
            @pl.loop(0, len(fresh))
            def _(i):
                j = pick(i, fresh)

                @pl.when(near(*inner(j), step))
                def _():
                    multiply(j, step > SUMMED)

        old = [p for p in range(SIDE * SIDE) if p != LAST and BLOCK_AT[p] <= before]
        came = [
            (dz, side) for side in range(CORES) for h in range(CHIPS // 2 + 1)
            for dz in sorted({h, (CHIPS - h) % CHIPS}) if before < NEAR_AT[h][side] <= step
        ]
        if old and came:
            @pl.loop(0, len(came))
            def _(i):
                dz = pick(i, [c[0] for c in came])
                side = pick(i, [c[1] for c in came])
                j = met((dz, side))
                here = j == old[0]
                for p in old[1:]:
                    here = here | (j == p)

                @pl.when(here)
                def _():
                    multiply(j, step > SUMMED)

    def add_sums(step):
        fresh = [p for p in range(SIDE * SIDE) if BLOCK_AT[p] <= step]

        @pl.loop(0, len(fresh))
        def _(i):
            j = pick(i, fresh)
            dz, lane = inner(j)

            @pl.when(near(dz, lane, step))
            def _():
                block = col_panel[pl.ds(pl.multiple_of(j * rows, rows), rows)]
                psum[...] += jnp.dot(
                    row_panel[dz * CORES + lane, rows:], block, preferred_element_type=jnp.float32
                )

    def await_rows(count, sem):
        spot = col_panel.at[pl.ds(0, count)]
        pltpu.make_async_remote_copy(
            src_ref=spot, dst_ref=spot, send_sem=bulk_send.at[0], recv_sem=sem, device_id=neighbours[0]
        ).wait_recv()

    def take_xy(s):
        await_rows(4 * part, xy_recv.at[s])

    def take_z(s):
        if s < Z_SLOTS:
            await_rows(2 * part, z_recv.at[s])
            for (c, dz), at in sorted(Z_AT.items()):
                if at == s:
                    pair_copy(c, dz).start()

    def take_pair(h):
        await_rows(len({h, -h % CHIPS}) * rows, pair_recv.at[h])

    before = -1
    for s in range(SLOTS - 1):
        if s < SLOTS - 1:
            with jax.named_scope(f"xy{s}"):
                take_xy(s)
            for n in range(4):
                send(n, s + AHEAD)
        if 0 < s <= Z_LAG:
            with jax.named_scope(f"z{s - 1}"):
                take_z(s - 1)
        for n in (4, 5):
            if s > 0:
                send(n, s + AHEAD - 1)
        for h in range(CHIPS // 2):
            if s == NEAR_AT[h][1]:
                with jax.named_scope(f"pair{h}"):
                    take_pair(h)
        if s == Z_SLOTS - 1:
            with jax.named_scope(f"z{s}"):
                take_z(s)
        with jax.named_scope(f"sums{s}"):
            if s < 3:
                greeted(s, 1)
                if s < 2:
                    greet(s + 1, 1)
            if s == 3:
                send_block_sums()
            if s == SUMMED - 1:
                pass_block_sums()
            if s == SUMMED:
                take_block_sums()
                add_sums(before)
        if s in POINTS:
            with jax.named_scope(f"multiply{s}"):
                compute(s, before)
            before = s
        if s == Z_SLOTS - 2:
            with jax.named_scope("pair3"):
                take_pair(CHIPS // 2 - 1)
            with jax.named_scope("multiply3b"):
                compute(NEAR_AT[-2][1], before)
            before = NEAR_AT[-2][1]
        if Z_LAG <= s < Z_SLOTS - 1:
            with jax.named_scope(f"z{s}"):
                take_z(s)
            if s == Z_AT[DETOUR[0], CHIPS - DETOUR[1]]:
                @pl.when(z == 1)
                def _():
                    z_copy(*DETOUR, 1, detour_send.at[1], part // 2, part // 2).start()

    with jax.named_scope("multiplyA"):
        compute(NEAR_AT[-1][0], before)
    masks[1].wait()
    masks[2].wait()
    kept = keep_ref[...].astype(jnp.float32)
    level = 0.125 * thr_ref[...].astype(jnp.float32)
    far = met((CHIPS // 2, 1))
    for turn in range(CORES):
        with jax.named_scope(f"last{turn}"):
            @pl.when(core == turn)
            def _():
                take_pair(CHIPS // 2)

            @pl.when(core != turn)
            def _():
                take_xy(SLOTS - 1)
        if turn == 0:
            @pl.when(far != LAST)
            def _():
                multiply((1 - core) * far + core * LAST, True)
    final = core * far + (1 - core) * LAST
    dz, lane = inner(final)
    slot = dz * CORES + lane
    block = col_panel[pl.ds(pl.multiple_of(final * rows, rows), rows)]
    lines = psum[...] + jnp.dot(row_panel[slot, rows:], block, preferred_element_type=jnp.float32)
    cut = level * ((lines[2:3] + lines[1:2] + lines[0:1]) / order)
    parts = [jnp.zeros((1, TB), jnp.float32) for _ in range(cols // TB)]
    for lo in range(0, rows, TB):
        term = jnp.dot(row_panel[slot, lo : lo + TB], block, preferred_element_type=jnp.float32)
        for b in range(cols // TB):
            r, c = slice(lo, lo + TB), slice(b * TB, (b + 1) * TB)
            keep = jnp.broadcast_to(kept[lo // TB : lo // TB + 1, b : b + 1], (TB, TB))
            pruned = jnp.maximum(acc[r, c] + term[:, c] - cut[:, c], 0.0) * keep
            acc[r, c] = pruned
            parts[b] += jnp.sum(pruned, axis=0, keepdims=True)
    sums[0] = jnp.concatenate(parts, axis=1)

    totals, totals_all = spread(sums, 2, SIDE * SIDE, by_row)
    for copy in totals:
        copy.start()

    for k, count in enumerate((4 * SLOTS * part, (2 * Z_SLOTS - 1) * part + CHIPS * rows)):
        spot = col_panel.at[pl.ds(0, count)]
        pltpu.make_async_remote_copy(
            src_ref=spot, dst_ref=spot, send_sem=bulk_send.at[k], recv_sem=bulk_send.at[k],
            device_id=neighbours[0],
        ).wait_send()

    for n, sends, count in ((0, z != CHIPS - 1, part), (0, z == CHIPS - 1, part // 2), (1, z == 1, part // 2)):
        @pl.when(sends)
        def _():
            z_copy(*DETOUR, n, detour_send.at[n], 0, count).wait_send()

    with jax.named_scope("totals"):
        totals_all.wait_send()
        totals_all.wait_recv()
    total = sums[0]
    for i in range(1, SIDE * SIDE):
        total += sums[i]
    scale_ref[...] = 1.0 / jnp.maximum(total / order, 0.1)


def on_device(values, tile_mask, keep_mask, thr_index):
    rows, cols = values.shape
    dma, plain = pltpu.SemaphoreType.DMA, pltpu.SemaphoreType.REGULAR
    vmem, anywhere = pl.BlockSpec(memory_space=pltpu.VMEM), pl.BlockSpec(memory_space=pl.ANY)
    blocks = SIDE * SIDE
    pruned, scale = pl.pallas_call(
        kernel,
        out_shape=(pltpu.VMEM((rows, cols), jnp.float32), pltpu.VMEM((1, cols), jnp.float32)),
        in_specs=[anywhere] * 4,
        out_specs=(vmem, vmem),
        scratch_shapes=[
            pltpu.VMEM((CHIPS * CORES, rows + EXTRA, cols), jnp.bfloat16),
            pltpu.VMEM((blocks * rows, cols), jnp.bfloat16),
            pltpu.VMEM((rows, cols), jnp.bfloat16),
            pltpu.VMEM(tile_mask.shape, jnp.int32),
            pltpu.VMEM(keep_mask.shape, jnp.int32),
            pltpu.VMEM((1, cols), jnp.int32),
            pltpu.VMEM((blocks, 1, cols), jnp.float32),
            pltpu.VMEM((CHIPS * CORES, 1, cols), jnp.float32),
            pltpu.VMEM((blocks, 1, cols), jnp.float32),
            pltpu.VMEM((EXTRA, cols), jnp.float32),
            dma((2,)),
            dma((SLOTS,)),
            dma((Z_SLOTS,)),
            dma((CHIPS // 2 + 1,)),
            dma((2,)),
            dma((1,)),
            dma((4,)),
            dma((CHUNKS + 3,)),
            plain((7,)),
            plain((4,)),
        ],
        compiler_params=pltpu.CompilerParams(
            collective_id=0, has_side_effects=True,
            vmem_limit_bytes=63 * 2**20 - 4 * rows * cols + 2**19,
        ),
    )(values, tile_mask, keep_mask, thr_index.reshape(1, cols))
    return (pruned * scale).astype(jnp.bfloat16)


def solution(mesh):
    return jax.shard_map(
        on_device,
        mesh=mesh,
        in_specs=(P("row", "col"), P("row", "col"), P("row", "col"), P("col")),
        out_specs=P("row", "col"),
        check_vma=False,
    )
```

```python
import functools

import jax
import jax.numpy as jnp
from jax import lax
from jax.experimental import pallas as pl
from jax.experimental.pallas import tpu as pltpu
from jax.sharding import PartitionSpec as P

TB = 128
CORES = 2
SIDE = 4
CHIPS = 8
CHUNKS = 4
LAST = 10
EXTRA = 16
LINKS = ((1, 0), (-1, 0), (0, 1), (0, -1))

ORDER = (
    ((0, 0), (1, 0), (2, 0), (3, 0), (0, 4), (2, 3), (3, 3), (2, 4), (2, 1), (3, 1), (2, 2), (3, 2), (2, 5), (2, 7), (2, 6)),
    ((1, 0), (0, 0), (3, 0), (2, 0), (1, 12), (3, 1), (2, 1), (3, 12), (3, 3), (2, 3), (3, 2), (2, 2), (3, 13), (3, 15), (3, 14)),
    ((2, 0), (3, 0), (0, 0), (1, 0), (2, 1), (0, 12), (1, 12), (0, 4), (0, 1), (1, 4), (0, 8), (0, 13), (1, 8), (0, 5), (0, 9)),
    ((3, 0), (2, 0), (1, 0), (0, 0), (3, 3), (1, 4), (0, 4), (1, 12), (1, 3), (0, 12), (1, 8), (1, 15), (1, 7), (0, 8), (1, 11)),
)
SLOTS = len(ORDER[0])
Z_ORDER = (
    tuple((c, hop) for hop in range(3) for c in (1, 0, 2, 3)) + ((1, 3), (0, 3)),
    tuple((c, hop) for hop in range(3) for c in (2, 3, 0, 1)) + ((2, 3), (3, 3)),
)
DETOUR = (0, 3)
Z_SLOTS = len(Z_ORDER[0])
AHEAD = 4
POINTS = (3, 5, 7, 9, 11, 12, 13)
SUMMED = 10


def shift(place, link):
    dx, dy = LINKS[link]
    return (place // SIDE + dx) % SIDE * SIDE + (place % SIDE + dy) % SIDE


def arrivals():
    xy = {(c, shift(p, n)): s for n in range(4) for s, (c, p) in enumerate(ORDER[n])}
    z = {}
    for n, sign in ((0, 1), (1, -1)):
        for s, (c, hop) in enumerate(Z_ORDER[n]):
            z[c, sign * (hop + 1) % CHIPS] = s
    return xy, z


XY_AT, Z_AT = arrivals()
BLOCK_AT = {p: max(XY_AT[c, p] for c in range(CHUNKS)) for p in range(1, SIDE * SIDE)} | {0: 0}
Z_LAG = 10
NEAR_AT = [(-1, 0), (4, 5), (8, 9), (11.5, 12.5), (13.6, 13.8)]


def kernel(
    v_hbm, tile_hbm, keep_hbm, thr_hbm, acc, scale_ref,
    row_panel, col_panel, loaded, tile_ref, keep_ref, thr_ref, colsum, stats, sums, psum,
    bulk_send, xy_recv, z_recv, pair_recv,
    detour_send, small_send, small_recv, load_sem, ready, hello,
):
    rows, cols = v_hbm.shape
    part = rows // CHUNKS
    order = rows * SIDE * SIDE
    me_row, me_col = lax.axis_index("row"), lax.axis_index("col")
    x, y = me_row // SIDE, me_row % SIDE
    z, core = me_col // CORES, me_col % CORES

    def xy_device(dx, dy):
        return {"row": (x + dx + SIDE) % SIDE * SIDE + (y + dy + SIDE) % SIDE}

    def z_device(dz, lane=0):
        return {"col": (z + dz + CHIPS) % CHIPS * CORES + (core if lane == 0 else 1 - core)}

    neighbours = [xy_device(*link) for link in LINKS] + [z_device(1), z_device(-1), z_device(0, 1)]
    later = [x < SIDE - 1, x == 0, y < SIDE - 1, y == 0, z < CHIPS - 1, z == 0, core == 1]
    barrier = pltpu.get_barrier_semaphore()
    earlier = 0
    for n, device in enumerate(neighbours):
        earlier = earlier + 1 - later[n].astype(jnp.int32)

        @pl.when(later[n])
        def _():
            pl.semaphore_signal(barrier, inc=1, device_id=device)

    def load(q):
        spot = pl.ds(q * part, part)
        return pltpu.make_async_copy(v_hbm.at[spot], loaded.at[spot], load_sem.at[q])

    masks = (
        pltpu.make_async_copy(tile_hbm, tile_ref, load_sem.at[CHUNKS]),
        pltpu.make_async_copy(keep_hbm, keep_ref, load_sem.at[CHUNKS + 1]),
        pltpu.make_async_copy(thr_hbm, thr_ref, load_sem.at[CHUNKS + 2]),
    )
    masks[0].start()
    for q in range(CHUNKS):
        load(q).start()
    masks[1].start()
    masks[2].start()

    def xy_copy(c, place, n):
        to = shift(place, n)
        return pltpu.make_async_remote_copy(
            src_ref=col_panel.at[pl.ds(place * rows + c * part, part)],
            dst_ref=col_panel.at[pl.ds(to * rows + c * part, part)],
            send_sem=bulk_send.at[0], recv_sem=xy_recv.at[XY_AT[c, to]],
            device_id=neighbours[n],
        )

    def z_copy(c, hop, n, sent=None, lo=0, count=part):
        sign = 1 - 2 * n
        spot = pl.ds(c * part + lo, count)
        to = sign * (hop + 1) % CHIPS
        return pltpu.make_async_remote_copy(
            src_ref=row_panel.at[sign * hop % CHIPS * CORES, spot],
            dst_ref=row_panel.at[to * CORES, spot],
            send_sem=bulk_send.at[1] if sent is None else sent, recv_sem=z_recv.at[Z_AT[c, to]],
            device_id=neighbours[4 + n],
        )

    def pair_copy(c, dz):
        spot = pl.ds(c * part, part)
        return pltpu.make_async_remote_copy(
            src_ref=row_panel.at[dz * CORES, spot], dst_ref=row_panel.at[dz * CORES + 1, spot],
            send_sem=bulk_send.at[1],
            recv_sem=pair_recv.at[CHIPS // 2 + 1 if Z_AT.get((c, dz)) == Z_SLOTS - 1 else min(dz, CHIPS - dz)],
            device_id=neighbours[6],
        )

    def send(n, s):
        if n < 4 and s < SLOTS:
            xy_copy(*ORDER[n][s], n).start()
        elif n == 6 and s < CHUNKS:
            pair_copy(s, 0).start()
        elif n in (4, 5) and s < Z_SLOTS:
            if n == 4 and Z_ORDER[0][s] == DETOUR:
                @pl.when(z != CHIPS - 1)
                def _():
                    z_copy(*DETOUR, 0, detour_send.at[0]).start()

                @pl.when(z == CHIPS - 1)
                def _():
                    z_copy(*DETOUR, 0, detour_send.at[0], 0, part // 2).start()
            else:
                z_copy(*Z_ORDER[n - 4][s], n - 4).start()

    @pl.when(earlier > 0)
    def _():
        pl.semaphore_wait(barrier, earlier)

    for n, device in enumerate(neighbours):
        @pl.when(jnp.logical_not(later[n]))
        def _():
            pl.semaphore_signal(ready.at[n ^ 1 if n < 6 else n], inc=1, device_id=device)

    masks[0].wait()
    stored = tile_ref[...].astype(jnp.float32)
    for q in range(CHUNKS):
        load(q).wait()
        for lo in range(q * part, (q + 1) * part, TB):
            for b in range(cols // TB):
                r, c = slice(lo, lo + TB), slice(b * TB, (b + 1) * TB)
                i = lo // TB
                factor = jnp.broadcast_to(stored[i : i + 1, b : b + 1], (EXTRA, TB)).astype(jnp.bfloat16)
                tile = loaded[r, c] * jnp.concatenate([factor] * (TB // EXTRA), axis=0)
                row_panel[0, r, c] = tile
                col_panel[r, c] = tile

    def when_not(n, do):
        @pl.when(jnp.logical_not(later[n]))
        def _():
            do()

    for s in range(AHEAD - 1):
        for n in range(6):
            when_not(n, lambda: send(n, s))
    def open_late(n):
        @pl.when(later[n])
        def _():
            with jax.named_scope(f"open{n}"):
                pl.semaphore_wait(ready.at[n], 1)
            for s in range(CHUNKS if n == 6 else AHEAD - (n != 5)):
                send(n, s)

    when_not(6, lambda: [send(6, s) for s in range(CHUNKS)])
    for n in (6, 0, 2, 4, 1, 3):
        open_late(n)

    def greet(k, over):
        for device in neighbours[4 * over : 4 + 3 * over]:
            pl.semaphore_signal(hello.at[2 * over + k % 2], inc=1, device_id=device)

    def greeted(k, over):
        pl.semaphore_wait(hello.at[2 * over + k % 2], 4 - over)

    greet(0, 0)

    def spread(buffer, k, count, device):
        def copy(d):
            return pltpu.make_async_remote_copy(
                src_ref=buffer.at[0], dst_ref=buffer.at[d],
                send_sem=small_send.at[0], recv_sem=small_recv.at[k], device_id=device(d),
            )

        everything = pltpu.make_async_remote_copy(
            src_ref=buffer.at[pl.ds(1, count - 1)], dst_ref=buffer.at[pl.ds(1, count - 1)],
            send_sem=small_send.at[0], recv_sem=small_recv.at[k], device_id=neighbours[6],
        )
        def far(d):
            return min(d // SIDE, SIDE - d // SIDE) + min(d % SIDE, SIDE - d % SIDE)

        return [copy(d) for d in sorted(range(1, count), key=far, reverse=True)], everything

    def by_row(d):
        return xy_device(d // SIDE, d % SIDE)

    def by_col(d):
        return z_device(d)

    column_sums, column_sums_all = spread(colsum, 0, SIDE * SIDE, by_row)

    total = jnp.zeros((1, cols), jnp.float32)
    for lo in range(0, rows, TB):
        block = col_panel[lo : lo + TB].astype(jnp.float32)
        total += jnp.sum(block, axis=0, keepdims=True)
    colsum[0] = total
    acc[...] = jnp.zeros((rows, cols), jnp.float32)
    psum[...] = jnp.zeros((EXTRA, cols), jnp.float32)
    with jax.named_scope("greet"):
        for k in range(3):
            greeted(k, 0)
            if k < 2:
                greet(k + 1, 0)
    for copy in column_sums:
        copy.start()
    for n in range(5):
        send(n, AHEAD - 1)
    when_not(5, lambda: send(5, AHEAD - 1))
    open_late(5)
    greet(0, 1)

    block_sums, block_sums_all = spread(stats, 1, CHIPS, by_col)

    def send_block_sums():
        column_sums_all.wait_recv()
        column_sums_all.wait_send()
        total = colsum[0]
        for i in range(1, SIDE * SIDE):
            total += colsum[i]
        stats[0] = total
        for copy in block_sums:
            copy.start()

    pair_sums = pltpu.make_async_remote_copy(
        src_ref=stats.at[pl.ds(0, CHIPS)], dst_ref=stats.at[pl.ds(CHIPS, CHIPS)],
        send_sem=small_send.at[0], recv_sem=small_recv.at[3], device_id=neighbours[6],
    )

    def pass_block_sums():
        block_sums_all.wait_recv()
        block_sums_all.wait_send()
        pair_sums.start()

    def take_block_sums():
        pair_sums.wait()
        line = lax.broadcasted_iota(jnp.int32, (EXTRA, cols), 0)

        @pl.loop(0, CHIPS * CORES)
        def _(i):
            rest, spot = stats[i], jnp.zeros((EXTRA, cols), jnp.float32)
            for k in range(3):
                term = rest.astype(jnp.bfloat16).astype(jnp.float32)
                rest = rest - term
                spot = jnp.where(line == k, jnp.broadcast_to(term, (EXTRA, cols)), spot)
            row_panel[i % CHIPS * CORES + i // CHIPS, rows:] = spot.astype(jnp.bfloat16)

    def inner(j):
        k = (x - j // SIDE + SIDE) % SIDE * SIDE + (y - j % SIDE + SIDE) % SIDE
        dz = (z - k // CORES + CHIPS) % CHIPS
        lane = (core + k) % CORES
        return dz, lane

    def near(dz, lane, step):
        there = None
        for side in range(CORES):
            reach = max([h for h in range(CHIPS // 2 + 1) if NEAR_AT[h][side] <= step], default=-1)
            one = (lane == side) & ((dz <= reach) | (dz >= CHIPS - reach))
            there = one if there is None else there | one
        return there

    def pick(i, values):
        found = values[0]
        for k, value in enumerate(values[1:], 1):
            found = found + (i == k).astype(jnp.int32) * (value - values[0])
        return found

    def met(of):
        dz, side = of
        k = (z - dz + CHIPS) % CHIPS * CORES + (core + side) % CORES
        return (x - k // SIDE + SIDE) % SIDE * SIDE + (y - k % SIDE + SIDE) % SIDE

    def multiply(blocks, summed):
        term = None
        for j in blocks:
            dz, lane = inner(j)
            left = row_panel[dz * CORES + lane] if summed else row_panel[dz * CORES + lane, :rows]
            right = col_panel[pl.ds(pl.multiple_of(j * rows, rows), rows)]
            one = jnp.dot(left, right, preferred_element_type=jnp.float32)
            term = one if term is None else term + one
        acc[...] += term[:rows]
        if summed:
            psum[...] += term[rows:]

    def multiply_those(found, summed):
        (first, one), (second, other) = found

        @pl.when(one & other)
        def _():
            multiply((first, second), summed)

        @pl.when(one ^ other)
        def _():
            multiply((jnp.where(one, first, second),), summed)

    def compute(step, before):
        fresh = [p for p in range(SIDE * SIDE) if p != LAST and before < BLOCK_AT[p] <= step]
        if len(fresh) == 2:
            multiply_those([(p, near(*inner(p), step)) for p in fresh], step > SUMMED)
        elif fresh:
            @pl.loop(0, len(fresh))
            def _(i):
                j = pick(i, fresh)

                @pl.when(near(*inner(j), step))
                def _():
                    multiply((j,), step > SUMMED)

        old = [p for p in range(SIDE * SIDE) if p != LAST and BLOCK_AT[p] <= before]
        came = [
            (dz, side) for side in range(CORES) for h in range(CHIPS // 2 + 1)
            for dz in sorted({h, (CHIPS - h) % CHIPS}) if before < NEAR_AT[h][side] <= step
        ]
        def there(of):
            j = met(of)
            here = j == old[0]
            for p in old[1:]:
                here = here | (j == p)
            return j, here

        if old and len(came) == 2:
            multiply_those([there(of) for of in came], step > SUMMED)
        elif old and came:
            @pl.loop(0, len(came))
            def _(i):
                dz = pick(i, [c[0] for c in came])
                side = pick(i, [c[1] for c in came])
                j, here = there((dz, side))

                @pl.when(here)
                def _():
                    multiply((j,), step > SUMMED)

    def add_sums(step):
        fresh = [p for p in range(SIDE * SIDE) if BLOCK_AT[p] <= step]

        @pl.loop(0, len(fresh))
        def _(i):
            j = pick(i, fresh)
            dz, lane = inner(j)

            @pl.when(near(dz, lane, step))
            def _():
                block = col_panel[pl.ds(pl.multiple_of(j * rows, rows), rows)]
                psum[...] += jnp.dot(
                    row_panel[dz * CORES + lane, rows:], block, preferred_element_type=jnp.float32
                )

    def await_rows(count, sem):
        spot = col_panel.at[pl.ds(0, count)]
        pltpu.make_async_remote_copy(
            src_ref=spot, dst_ref=spot, send_sem=bulk_send.at[0], recv_sem=sem, device_id=neighbours[0]
        ).wait_recv()

    def take_xy(s):
        await_rows(4 * part, xy_recv.at[s])

    def take_z(s):
        if s < Z_SLOTS:
            await_rows(2 * part, z_recv.at[s])
            for (c, dz), at in sorted(Z_AT.items()):
                if at == s:
                    pair_copy(c, dz).start()

    def take_pair(h):
        await_rows(rows // 2 if h >= CHIPS // 2 else rows if h == 0 else 2 * rows, pair_recv.at[h])

    before = -1
    for s in range(SLOTS - 1):
        if s < SLOTS - 1:
            if s == Z_SLOTS - 1:
                @pl.when(z != 0)
                def _():
                    with jax.named_scope(f"z{s}"):
                        take_z(s)
            with jax.named_scope(f"xy{s}"):
                take_xy(s)
            for n in range(4):
                send(n, s + AHEAD)
        if 0 < s <= Z_LAG:
            with jax.named_scope(f"z{s - 1}"):
                take_z(s - 1)
        for n in (4, 5):
            if s > 0:
                send(n, s + AHEAD - 1)
        for h in range(CHIPS // 2):
            if s == NEAR_AT[h][1]:
                with jax.named_scope(f"pair{h}"):
                    take_pair(h)
        if s == Z_SLOTS - 1:
            @pl.when(z == 0)
            def _():
                take_z(s)
        with jax.named_scope(f"sums{s}"):
            if s < 3:
                greeted(s, 1)
                if s < 2:
                    greet(s + 1, 1)
            if s == 3:
                send_block_sums()
            if s == SUMMED - 1:
                pass_block_sums()
            if s == SUMMED:
                take_block_sums()
                add_sums(before)
        if s in POINTS:
            with jax.named_scope(f"multiply{s}"):
                compute(s, before)
            before = s
        if s == Z_SLOTS - 2:
            with jax.named_scope("pair3"):
                take_pair(CHIPS // 2 - 1)
            with jax.named_scope("multiply3b"):
                compute(NEAR_AT[-2][1], before)
            before = NEAR_AT[-2][1]
        if Z_LAG <= s < Z_SLOTS - 1:
            with jax.named_scope(f"z{s}"):
                take_z(s)
            if s == Z_AT[DETOUR[0], CHIPS - DETOUR[1]]:
                @pl.when(z == 1)
                def _():
                    z_copy(*DETOUR, 1, detour_send.at[1], part // 2, part // 2).start()

    with jax.named_scope("multiplyA"):
        compute(NEAR_AT[-1][0], before)
    masks[1].wait()
    masks[2].wait()
    kept = keep_ref[...].astype(jnp.float32)
    level = 0.125 * thr_ref[...].astype(jnp.float32)
    far = met((CHIPS // 2, 1))
    for turn in range(CORES):
        with jax.named_scope(f"last{turn}"):
            @pl.when(core == turn)
            def _():
                take_pair(CHIPS // 2)
                if turn == 0:
                    take_pair(CHIPS // 2 + 1)

            @pl.when(core != turn)
            def _():
                take_xy(SLOTS - 1)
        if turn == 0:
            @pl.when(far != LAST)
            def _():
                multiply(((1 - core) * far + core * LAST,), True)
    final = core * far + (1 - core) * LAST
    dz, lane = inner(final)
    slot = dz * CORES + lane
    block = col_panel[pl.ds(pl.multiple_of(final * rows, rows), rows)]
    lines = psum[...] + jnp.dot(row_panel[slot, rows:], block, preferred_element_type=jnp.float32)
    cut = level * ((lines[2:3] + lines[1:2] + lines[0:1]) / order)
    parts = [jnp.zeros((1, TB), jnp.float32) for _ in range(cols // TB)]
    late = sorted(c for c in range(CHUNKS) if Z_AT[c, CHIPS // 2] == Z_SLOTS - 1)
    for q in sorted(range(CHUNKS), key=lambda c: c in late):
        if q == late[0]:
            with jax.named_scope("last2"):
                @pl.when(core == 1)
                def _():
                    take_pair(CHIPS // 2 + 1)
        lo = q * TB
        term = jnp.dot(row_panel[slot, lo : lo + TB], block, preferred_element_type=jnp.float32)
        for b in range(cols // TB):
            r, c = slice(lo, lo + TB), slice(b * TB, (b + 1) * TB)
            keep = jnp.broadcast_to(kept[lo // TB : lo // TB + 1, b : b + 1], (TB, TB))
            pruned = jnp.maximum(acc[r, c] + term[:, c] - cut[:, c], 0.0) * keep
            acc[r, c] = pruned
            parts[b] += jnp.sum(pruned, axis=0, keepdims=True)
    sums[0] = jnp.concatenate(parts, axis=1)

    totals, totals_all = spread(sums, 2, SIDE * SIDE, by_row)
    for copy in totals:
        copy.start()

    for k, count in enumerate((4 * SLOTS * part, (2 * Z_SLOTS - 1) * part + CHIPS * rows)):
        spot = col_panel.at[pl.ds(0, count)]
        pltpu.make_async_remote_copy(
            src_ref=spot, dst_ref=spot, send_sem=bulk_send.at[k], recv_sem=bulk_send.at[k],
            device_id=neighbours[0],
        ).wait_send()

    for n, sends, count in ((0, z != CHIPS - 1, part), (0, z == CHIPS - 1, part // 2), (1, z == 1, part // 2)):
        @pl.when(sends)
        def _():
            z_copy(*DETOUR, n, detour_send.at[n], 0, count).wait_send()

    with jax.named_scope("totals"):
        totals_all.wait_send()
        totals_all.wait_recv()
    total = sums[0]
    for i in range(1, SIDE * SIDE):
        total += sums[i]
    scale_ref[...] = 1.0 / jnp.maximum(total / order, 0.1)


def on_device(values, tile_mask, keep_mask, thr_index):
    rows, cols = values.shape
    dma, plain = pltpu.SemaphoreType.DMA, pltpu.SemaphoreType.REGULAR
    vmem, anywhere = pl.BlockSpec(memory_space=pltpu.VMEM), pl.BlockSpec(memory_space=pl.ANY)
    blocks = SIDE * SIDE
    pruned, scale = pl.pallas_call(
        kernel,
        out_shape=(pltpu.VMEM((rows, cols), jnp.float32), pltpu.VMEM((1, cols), jnp.float32)),
        in_specs=[anywhere] * 4,
        out_specs=(vmem, vmem),
        scratch_shapes=[
            pltpu.VMEM((CHIPS * CORES, rows + EXTRA, cols), jnp.bfloat16),
            pltpu.VMEM((blocks * rows, cols), jnp.bfloat16),
            pltpu.VMEM((rows, cols), jnp.bfloat16),
            pltpu.VMEM(tile_mask.shape, jnp.int32),
            pltpu.VMEM(keep_mask.shape, jnp.int32),
            pltpu.VMEM((1, cols), jnp.int32),
            pltpu.VMEM((blocks, 1, cols), jnp.float32),
            pltpu.VMEM((CHIPS * CORES, 1, cols), jnp.float32),
            pltpu.VMEM((blocks, 1, cols), jnp.float32),
            pltpu.VMEM((EXTRA, cols), jnp.float32),
            dma((2,)),
            dma((SLOTS,)),
            dma((Z_SLOTS,)),
            dma((CHIPS // 2 + 2,)),
            dma((2,)),
            dma((1,)),
            dma((4,)),
            dma((CHUNKS + 3,)),
            plain((7,)),
            plain((4,)),
        ],
        compiler_params=pltpu.CompilerParams(
            collective_id=0, has_side_effects=True,
            vmem_limit_bytes=63 * 2**20 - 4 * rows * cols + 2**19,
        ),
    )(values, tile_mask, keep_mask, thr_index.reshape(1, cols))
    return (pruned * scale).astype(jnp.bfloat16)


def solution(mesh):
    return jax.shard_map(
        on_device,
        mesh=mesh,
        in_specs=(P("row", "col"), P("row", "col"), P("row", "col"), P("col")),
        out_specs=P("row", "col"),
        check_vma=False,
    )
```

```python
import functools

import jax
import jax.numpy as jnp
from jax import lax
from jax.experimental import pallas as pl
from jax.experimental.pallas import tpu as pltpu
from jax.sharding import PartitionSpec as P

TB = 128
CORES = 2
SIDE = 4
CHIPS = 8
CHUNKS = 4
LAST = 10
EXTRA = 16
LINKS = ((1, 0), (-1, 0), (0, 1), (0, -1))

ORDER = (
    ((0, 0), (1, 0), (2, 0), (3, 0), (0, 4), (2, 3), (3, 3), (2, 4), (2, 1), (3, 1), (2, 2), (3, 2), (2, 5), (2, 7), (2, 6)),
    ((1, 0), (0, 0), (3, 0), (2, 0), (1, 12), (3, 1), (2, 1), (3, 12), (3, 3), (2, 3), (3, 2), (2, 2), (3, 13), (3, 15), (3, 14)),
    ((2, 0), (3, 0), (0, 0), (1, 0), (2, 1), (0, 12), (1, 12), (0, 4), (0, 1), (1, 4), (0, 8), (0, 13), (1, 8), (0, 5), (0, 9)),
    ((3, 0), (2, 0), (1, 0), (0, 0), (3, 3), (1, 4), (0, 4), (1, 12), (1, 3), (0, 12), (1, 8), (1, 15), (1, 7), (0, 8), (1, 11)),
)
SLOTS = len(ORDER[0])
Z_ORDER = (
    tuple((c, hop) for hop in range(3) for c in (1, 0, 2, 3)) + ((1, 3), (0, 3)),
    tuple((c, hop) for hop in range(3) for c in (2, 3, 0, 1)) + ((2, 3), (3, 3)),
)
DETOUR = (0, 3)
Z_SLOTS = len(Z_ORDER[0])
AHEAD = 4
POINTS = (3, 5, 7, 9, 11, 12, 13)
SUMMED = 10


def shift(place, link):
    dx, dy = LINKS[link]
    return (place // SIDE + dx) % SIDE * SIDE + (place % SIDE + dy) % SIDE


def arrivals():
    xy = {(c, shift(p, n)): s for n in range(4) for s, (c, p) in enumerate(ORDER[n])}
    z = {}
    for n, sign in ((0, 1), (1, -1)):
        for s, (c, hop) in enumerate(Z_ORDER[n]):
            z[c, sign * (hop + 1) % CHIPS] = s
    return xy, z


XY_AT, Z_AT = arrivals()
BLOCK_AT = {p: max(XY_AT[c, p] for c in range(CHUNKS)) for p in range(1, SIDE * SIDE)} | {0: 0}
Z_LAG = 10
NEAR_AT = [(-1, 0), (4, 5), (8, 9), (11.5, 12.5), (13.6, 13.8)]


def kernel(
    v_hbm, tile_hbm, keep_hbm, thr_hbm, acc, scale_ref,
    row_panel, col_panel, loaded, tile_ref, keep_ref, thr_ref, colsum, stats, sums, psum,
    bulk_send, xy_recv, z_recv, pair_recv,
    detour_send, small_send, small_recv, load_sem, ready, hello,
):
    rows, cols = v_hbm.shape
    part = rows // CHUNKS
    order = rows * SIDE * SIDE
    me_row, me_col = lax.axis_index("row"), lax.axis_index("col")
    x, y = me_row // SIDE, me_row % SIDE
    z, core = me_col // CORES, me_col % CORES

    def xy_device(dx, dy):
        return {"row": (x + dx + SIDE) % SIDE * SIDE + (y + dy + SIDE) % SIDE}

    def z_device(dz, lane=0):
        return {"col": (z + dz + CHIPS) % CHIPS * CORES + (core if lane == 0 else 1 - core)}

    neighbours = [xy_device(*link) for link in LINKS] + [z_device(1), z_device(-1), z_device(0, 1)]
    later = [x < SIDE - 1, x == 0, y < SIDE - 1, y == 0, z < CHIPS - 1, z == 0, core == 1]
    barrier = pltpu.get_barrier_semaphore()
    earlier = 0
    for n, device in enumerate(neighbours):
        earlier = earlier + 1 - later[n].astype(jnp.int32)

        @pl.when(later[n])
        def _():
            pl.semaphore_signal(barrier, inc=1, device_id=device)

    def load(q):
        spot = pl.ds(q * part, part)
        return pltpu.make_async_copy(v_hbm.at[spot], loaded.at[spot], load_sem.at[q])

    masks = (
        pltpu.make_async_copy(tile_hbm, tile_ref, load_sem.at[CHUNKS]),
        pltpu.make_async_copy(keep_hbm, keep_ref, load_sem.at[CHUNKS + 1]),
        pltpu.make_async_copy(thr_hbm, thr_ref, load_sem.at[CHUNKS + 2]),
    )
    masks[0].start()
    for q in range(CHUNKS):
        load(q).start()
    masks[1].start()
    masks[2].start()

    def xy_copy(c, place, n):
        to = shift(place, n)
        return pltpu.make_async_remote_copy(
            src_ref=col_panel.at[pl.ds(place * rows + c * part, part)],
            dst_ref=col_panel.at[pl.ds(to * rows + c * part, part)],
            send_sem=bulk_send.at[0], recv_sem=xy_recv.at[XY_AT[c, to]],
            device_id=neighbours[n],
        )

    def z_copy(c, hop, n, sent=None, lo=0, count=part):
        sign = 1 - 2 * n
        spot = pl.ds(c * part + lo, count)
        to = sign * (hop + 1) % CHIPS
        return pltpu.make_async_remote_copy(
            src_ref=row_panel.at[sign * hop % CHIPS * CORES, spot],
            dst_ref=row_panel.at[to * CORES, spot],
            send_sem=bulk_send.at[1] if sent is None else sent, recv_sem=z_recv.at[Z_AT[c, to]],
            device_id=neighbours[4 + n],
        )

    def pair_copy(c, dz):
        spot = pl.ds(c * part, part)
        return pltpu.make_async_remote_copy(
            src_ref=row_panel.at[dz * CORES, spot], dst_ref=row_panel.at[dz * CORES + 1, spot],
            send_sem=bulk_send.at[1],
            recv_sem=pair_recv.at[CHIPS // 2 + 1 if Z_AT.get((c, dz)) == Z_SLOTS - 1 else min(dz, CHIPS - dz)],
            device_id=neighbours[6],
        )

    def send(n, s):
        if n < 4 and s < SLOTS:
            xy_copy(*ORDER[n][s], n).start()
        elif n == 6 and s < CHUNKS:
            pair_copy(s, 0).start()
        elif n in (4, 5) and s < Z_SLOTS:
            if n == 4 and Z_ORDER[0][s] == DETOUR:
                @pl.when(z != CHIPS - 1)
                def _():
                    z_copy(*DETOUR, 0, detour_send.at[0]).start()

                @pl.when(z == CHIPS - 1)
                def _():
                    z_copy(*DETOUR, 0, detour_send.at[0], 0, 32).start()
            else:
                z_copy(*Z_ORDER[n - 4][s], n - 4).start()

    @pl.when(earlier > 0)
    def _():
        pl.semaphore_wait(barrier, earlier)

    for n, device in enumerate(neighbours):
        @pl.when(jnp.logical_not(later[n]))
        def _():
            pl.semaphore_signal(ready.at[n ^ 1 if n < 6 else n], inc=1, device_id=device)

    masks[0].wait()
    stored = tile_ref[...].astype(jnp.float32)
    for q in range(CHUNKS):
        load(q).wait()
        for lo in range(q * part, (q + 1) * part, TB):
            for b in range(cols // TB):
                r, c = slice(lo, lo + TB), slice(b * TB, (b + 1) * TB)
                i = lo // TB
                factor = jnp.broadcast_to(stored[i : i + 1, b : b + 1], (EXTRA, TB)).astype(jnp.bfloat16)
                tile = loaded[r, c] * jnp.concatenate([factor] * (TB // EXTRA), axis=0)
                row_panel[0, r, c] = tile
                col_panel[r, c] = tile

    def when_not(n, do):
        @pl.when(jnp.logical_not(later[n]))
        def _():
            do()

    for s in range(AHEAD - 1):
        for n in range(6):
            when_not(n, lambda: send(n, s))
    def open_late(n):
        @pl.when(later[n])
        def _():
            with jax.named_scope(f"open{n}"):
                pl.semaphore_wait(ready.at[n], 1)
            for s in range(CHUNKS if n == 6 else AHEAD - (n != 5)):
                send(n, s)

    when_not(6, lambda: [send(6, s) for s in range(CHUNKS)])
    for n in (6, 0, 2, 4, 1, 3):
        open_late(n)

    def greet(k, over):
        for device in neighbours[4 * over : 4 + 3 * over]:
            pl.semaphore_signal(hello.at[2 * over + k % 2], inc=1, device_id=device)

    def greeted(k, over):
        pl.semaphore_wait(hello.at[2 * over + k % 2], 4 - over)

    greet(0, 0)

    def spread(buffer, k, count, device):
        def copy(d):
            return pltpu.make_async_remote_copy(
                src_ref=buffer.at[0], dst_ref=buffer.at[d],
                send_sem=small_send.at[0], recv_sem=small_recv.at[k], device_id=device(d),
            )

        everything = pltpu.make_async_remote_copy(
            src_ref=buffer.at[pl.ds(1, count - 1)], dst_ref=buffer.at[pl.ds(1, count - 1)],
            send_sem=small_send.at[0], recv_sem=small_recv.at[k], device_id=neighbours[6],
        )
        def far(d):
            return min(d // SIDE, SIDE - d // SIDE) + min(d % SIDE, SIDE - d % SIDE)

        return [copy(d) for d in sorted(range(1, count), key=far, reverse=True)], everything

    def by_row(d):
        return xy_device(d // SIDE, d % SIDE)

    def by_col(d):
        return z_device(d)

    column_sums, column_sums_all = spread(colsum, 0, SIDE * SIDE, by_row)

    total = jnp.zeros((1, cols), jnp.float32)
    for lo in range(0, rows, TB):
        block = col_panel[lo : lo + TB].astype(jnp.float32)
        total += jnp.sum(block, axis=0, keepdims=True)
    colsum[0] = total
    acc[...] = jnp.zeros((rows, cols), jnp.float32)
    psum[...] = jnp.zeros((EXTRA, cols), jnp.float32)
    with jax.named_scope("greet"):
        for k in range(3):
            greeted(k, 0)
            if k < 2:
                greet(k + 1, 0)
    for copy in column_sums:
        copy.start()
    for n in range(5):
        send(n, AHEAD - 1)
    when_not(5, lambda: send(5, AHEAD - 1))
    open_late(5)
    greet(0, 1)

    block_sums, block_sums_all = spread(stats, 1, CHIPS, by_col)

    def send_block_sums():
        column_sums_all.wait_recv()
        column_sums_all.wait_send()
        total = colsum[0]
        for i in range(1, SIDE * SIDE):
            total += colsum[i]
        stats[0] = total
        for copy in block_sums:
            copy.start()

    pair_sums = pltpu.make_async_remote_copy(
        src_ref=stats.at[pl.ds(0, CHIPS)], dst_ref=stats.at[pl.ds(CHIPS, CHIPS)],
        send_sem=small_send.at[0], recv_sem=small_recv.at[3], device_id=neighbours[6],
    )

    def pass_block_sums():
        block_sums_all.wait_recv()
        block_sums_all.wait_send()
        pair_sums.start()

    def take_block_sums():
        pair_sums.wait()
        line = lax.broadcasted_iota(jnp.int32, (EXTRA, cols), 0)

        @pl.loop(0, CHIPS * CORES)
        def _(i):
            rest, spot = stats[i], jnp.zeros((EXTRA, cols), jnp.float32)
            for k in range(3):
                term = rest.astype(jnp.bfloat16).astype(jnp.float32)
                rest = rest - term
                spot = jnp.where(line == k, jnp.broadcast_to(term, (EXTRA, cols)), spot)
            row_panel[i % CHIPS * CORES + i // CHIPS, rows:] = spot.astype(jnp.bfloat16)

    def inner(j):
        k = (x - j // SIDE + SIDE) % SIDE * SIDE + (y - j % SIDE + SIDE) % SIDE
        dz = (z - k // CORES + CHIPS) % CHIPS
        lane = (core + k) % CORES
        return dz, lane

    def near(dz, lane, step):
        there = None
        for side in range(CORES):
            reach = max([h for h in range(CHIPS // 2 + 1) if NEAR_AT[h][side] <= step], default=-1)
            one = (lane == side) & ((dz <= reach) | (dz >= CHIPS - reach))
            there = one if there is None else there | one
        return there

    def pick(i, values):
        found = values[0]
        for k, value in enumerate(values[1:], 1):
            found = found + (i == k).astype(jnp.int32) * (value - values[0])
        return found

    def met(of):
        dz, side = of
        k = (z - dz + CHIPS) % CHIPS * CORES + (core + side) % CORES
        return (x - k // SIDE + SIDE) % SIDE * SIDE + (y - k % SIDE + SIDE) % SIDE

    def multiply(blocks, summed):
        term = None
        for j in blocks:
            dz, lane = inner(j)
            left = row_panel[dz * CORES + lane] if summed else row_panel[dz * CORES + lane, :rows]
            right = col_panel[pl.ds(pl.multiple_of(j * rows, rows), rows)]
            one = jnp.dot(left, right, preferred_element_type=jnp.float32)
            term = one if term is None else term + one
        acc[...] += term[:rows]
        if summed:
            psum[...] += term[rows:]

    def multiply_those(found, summed):
        (first, one), (second, other) = found

        @pl.when(one & other)
        def _():
            multiply((first, second), summed)

        @pl.when(one ^ other)
        def _():
            multiply((jnp.where(one, first, second),), summed)

    def compute(step, before):
        fresh = [p for p in range(SIDE * SIDE) if p != LAST and before < BLOCK_AT[p] <= step]
        if len(fresh) == 2:
            multiply_those([(p, near(*inner(p), step)) for p in fresh], step > SUMMED)
        elif fresh:
            @pl.loop(0, len(fresh))
            def _(i):
                j = pick(i, fresh)

                @pl.when(near(*inner(j), step))
                def _():
                    multiply((j,), step > SUMMED)

        old = [p for p in range(SIDE * SIDE) if p != LAST and BLOCK_AT[p] <= before]
        came = [
            (dz, side) for side in range(CORES) for h in range(CHIPS // 2 + 1)
            for dz in sorted({h, (CHIPS - h) % CHIPS}) if before < NEAR_AT[h][side] <= step
        ]
        def there(of):
            j = met(of)
            here = j == old[0]
            for p in old[1:]:
                here = here | (j == p)
            return j, here

        if old and len(came) == 2:
            multiply_those([there(of) for of in came], step > SUMMED)
        elif old and came:
            @pl.loop(0, len(came))
            def _(i):
                dz = pick(i, [c[0] for c in came])
                side = pick(i, [c[1] for c in came])
                j, here = there((dz, side))

                @pl.when(here)
                def _():
                    multiply((j,), step > SUMMED)

    def add_sums(step):
        fresh = [p for p in range(SIDE * SIDE) if BLOCK_AT[p] <= step]

        @pl.loop(0, len(fresh))
        def _(i):
            j = pick(i, fresh)
            dz, lane = inner(j)

            @pl.when(near(dz, lane, step))
            def _():
                block = col_panel[pl.ds(pl.multiple_of(j * rows, rows), rows)]
                psum[...] += jnp.dot(
                    row_panel[dz * CORES + lane, rows:], block, preferred_element_type=jnp.float32
                )

    def await_rows(count, sem):
        spot = col_panel.at[pl.ds(0, count)]
        pltpu.make_async_remote_copy(
            src_ref=spot, dst_ref=spot, send_sem=bulk_send.at[0], recv_sem=sem, device_id=neighbours[0]
        ).wait_recv()

    def take_xy(s):
        await_rows(4 * part, xy_recv.at[s])

    def take_z(s):
        if s < Z_SLOTS:
            await_rows(2 * part, z_recv.at[s])
            for (c, dz), at in sorted(Z_AT.items()):
                if at == s:
                    pair_copy(c, dz).start()

    def take_pair(h):
        await_rows(rows // 2 if h >= CHIPS // 2 else rows if h == 0 else 2 * rows, pair_recv.at[h])

    before = -1
    for s in range(SLOTS - 1):
        if s < SLOTS - 1:
            if s == Z_SLOTS - 1:
                with jax.named_scope(f"z{s}"):
                    take_z(s)
            with jax.named_scope(f"xy{s}"):
                take_xy(s)
            for n in range(4):
                send(n, s + AHEAD)
        if 0 < s <= Z_LAG:
            with jax.named_scope(f"z{s - 1}"):
                take_z(s - 1)
        for n in (4, 5):
            if s > 0:
                send(n, s + AHEAD - 1)
        for h in range(CHIPS // 2):
            if s == NEAR_AT[h][1]:
                with jax.named_scope(f"pair{h}"):
                    take_pair(h)
        with jax.named_scope(f"sums{s}"):
            if s < 3:
                greeted(s, 1)
                if s < 2:
                    greet(s + 1, 1)
            if s == 3:
                send_block_sums()
            if s == SUMMED - 1:
                pass_block_sums()
            if s == SUMMED:
                take_block_sums()
                add_sums(before)
        if s in POINTS:
            with jax.named_scope(f"multiply{s}"):
                compute(s, before)
            before = s
        if s == Z_SLOTS - 2:
            with jax.named_scope("pair3"):
                take_pair(CHIPS // 2 - 1)
            with jax.named_scope("multiply3b"):
                compute(NEAR_AT[-2][1], before)
            before = NEAR_AT[-2][1]
        if Z_LAG <= s < Z_SLOTS - 1:
            with jax.named_scope(f"z{s}"):
                take_z(s)
            if s == Z_AT[DETOUR[0], CHIPS - DETOUR[1]]:
                @pl.when(z == 1)
                def _():
                    z_copy(*DETOUR, 1, detour_send.at[1], 32, part - 32).start()

    near_last = met((CHIPS // 2, 0))
    with jax.named_scope("multiplyA"):
        @pl.when((core == 1) & (near_last != LAST))
        def _():
            multiply((near_last,), True)

    masks[1].wait()
    masks[2].wait()
    kept = keep_ref[...].astype(jnp.float32)
    level = 0.125 * thr_ref[...].astype(jnp.float32)
    far = met((CHIPS // 2, 1))
    for turn in range(CORES):
        with jax.named_scope(f"last{turn}"):
            @pl.when(core == turn)
            def _():
                take_pair(CHIPS // 2)
                if turn == 0:
                    take_pair(CHIPS // 2 + 1)

            @pl.when(core != turn)
            def _():
                take_xy(SLOTS - 1)
        if turn == 0:
            multiply_those([
                (near_last, (core == 0) & (near_last != LAST)),
                ((1 - core) * far + core * LAST, far != LAST),
            ], True)
    final = core * far + (1 - core) * LAST
    dz, lane = inner(final)
    slot = dz * CORES + lane
    block = col_panel[pl.ds(pl.multiple_of(final * rows, rows), rows)]
    lines = psum[...] + jnp.dot(row_panel[slot, rows:], block, preferred_element_type=jnp.float32)
    cut = level * ((lines[2:3] + lines[1:2] + lines[0:1]) / order)
    parts = [jnp.zeros((1, TB), jnp.float32) for _ in range(cols // TB)]
    late = sorted(c for c in range(CHUNKS) if Z_AT[c, CHIPS // 2] == Z_SLOTS - 1)
    for q in sorted(range(CHUNKS), key=lambda c: c in late):
        if q == late[0]:
            with jax.named_scope("last2"):
                @pl.when(core == 1)
                def _():
                    take_pair(CHIPS // 2 + 1)
        lo = q * TB
        term = jnp.dot(row_panel[slot, lo : lo + TB], block, preferred_element_type=jnp.float32)
        for b in range(cols // TB):
            r, c = slice(lo, lo + TB), slice(b * TB, (b + 1) * TB)
            keep = jnp.broadcast_to(kept[lo // TB : lo // TB + 1, b : b + 1], (TB, TB))
            pruned = jnp.maximum(acc[r, c] + term[:, c] - cut[:, c], 0.0) * keep
            acc[r, c] = pruned
            parts[b] += jnp.sum(pruned, axis=0, keepdims=True)
    sums[0] = jnp.concatenate(parts, axis=1)

    totals, totals_all = spread(sums, 2, SIDE * SIDE, by_row)
    for copy in totals:
        copy.start()

    for k, count in enumerate((4 * SLOTS * part, (2 * Z_SLOTS - 1) * part + CHIPS * rows)):
        spot = col_panel.at[pl.ds(0, count)]
        pltpu.make_async_remote_copy(
            src_ref=spot, dst_ref=spot, send_sem=bulk_send.at[k], recv_sem=bulk_send.at[k],
            device_id=neighbours[0],
        ).wait_send()

    for n, sends, count in ((0, z != CHIPS - 1, part), (0, z == CHIPS - 1, 32), (1, z == 1, part - 32)):
        @pl.when(sends)
        def _():
            z_copy(*DETOUR, n, detour_send.at[n], 0, count).wait_send()

    with jax.named_scope("totals"):
        totals_all.wait_send()
        totals_all.wait_recv()
    total = sums[0]
    for i in range(1, SIDE * SIDE):
        total += sums[i]
    scale_ref[...] = 1.0 / jnp.maximum(total / order, 0.1)


def on_device(values, tile_mask, keep_mask, thr_index):
    rows, cols = values.shape
    dma, plain = pltpu.SemaphoreType.DMA, pltpu.SemaphoreType.REGULAR
    vmem, anywhere = pl.BlockSpec(memory_space=pltpu.VMEM), pl.BlockSpec(memory_space=pl.ANY)
    blocks = SIDE * SIDE
    pruned, scale = pl.pallas_call(
        kernel,
        out_shape=(pltpu.VMEM((rows, cols), jnp.float32), pltpu.VMEM((1, cols), jnp.float32)),
        in_specs=[anywhere] * 4,
        out_specs=(vmem, vmem),
        scratch_shapes=[
            pltpu.VMEM((CHIPS * CORES, rows + EXTRA, cols), jnp.bfloat16),
            pltpu.VMEM((blocks * rows, cols), jnp.bfloat16),
            pltpu.VMEM((rows, cols), jnp.bfloat16),
            pltpu.VMEM(tile_mask.shape, jnp.int32),
            pltpu.VMEM(keep_mask.shape, jnp.int32),
            pltpu.VMEM((1, cols), jnp.int32),
            pltpu.VMEM((blocks, 1, cols), jnp.float32),
            pltpu.VMEM((CHIPS * CORES, 1, cols), jnp.float32),
            pltpu.VMEM((blocks, 1, cols), jnp.float32),
            pltpu.VMEM((EXTRA, cols), jnp.float32),
            dma((2,)),
            dma((SLOTS,)),
            dma((Z_SLOTS,)),
            dma((CHIPS // 2 + 2,)),
            dma((2,)),
            dma((1,)),
            dma((4,)),
            dma((CHUNKS + 3,)),
            plain((7,)),
            plain((4,)),
        ],
        compiler_params=pltpu.CompilerParams(
            collective_id=0, has_side_effects=True,
            vmem_limit_bytes=63 * 2**20 - 4 * rows * cols + 2**19,
        ),
    )(values, tile_mask, keep_mask, thr_index.reshape(1, cols))
    return (pruned * scale).astype(jnp.bfloat16)


def solution(mesh):
    return jax.shard_map(
        on_device,
        mesh=mesh,
        in_specs=(P("row", "col"), P("row", "col"), P("row", "col"), P("col")),
        out_specs=P("row", "col"),
        check_vma=False,
    )
```

```python
import functools

import jax
import jax.numpy as jnp
from jax import lax
from jax.experimental import pallas as pl
from jax.experimental.pallas import tpu as pltpu
from jax.sharding import PartitionSpec as P

TB = 128
CORES = 2
SIDE = 4
CHIPS = 8
CHUNKS = 4
LAST = 10
EXTRA = 16
LINKS = ((1, 0), (-1, 0), (0, 1), (0, -1))

ORDER = (
    ((0, 0), (1, 0), (2, 0), (3, 0), (0, 4), (2, 3), (3, 3), (2, 4), (2, 1), (3, 1), (2, 2), (3, 2), (2, 5), (2, 7), (2, 6)),
    ((1, 0), (0, 0), (3, 0), (2, 0), (1, 12), (3, 1), (2, 1), (3, 12), (3, 3), (2, 3), (3, 2), (2, 2), (3, 13), (3, 15), (3, 14)),
    ((2, 0), (3, 0), (0, 0), (1, 0), (2, 1), (0, 12), (1, 12), (0, 4), (0, 1), (1, 4), (0, 8), (0, 13), (1, 8), (0, 5), (0, 9)),
    ((3, 0), (2, 0), (1, 0), (0, 0), (3, 3), (1, 4), (0, 4), (1, 12), (1, 3), (0, 12), (1, 8), (1, 15), (1, 7), (0, 8), (1, 11)),
)
SLOTS = len(ORDER[0])
Z_ORDER = (
    tuple((c, hop) for hop in range(3) for c in (1, 0, 2, 3)) + ((1, 3), (0, 3)),
    tuple((c, hop) for hop in range(3) for c in (2, 3, 0, 1)) + ((2, 3), (3, 3)),
)
DETOUR = (0, 3)
Z_SLOTS = len(Z_ORDER[0])
AHEAD = 4
POINTS = (3, 5, 7, 9, 11, 12, 13)
SUMMED = 10


def shift(place, link):
    dx, dy = LINKS[link]
    return (place // SIDE + dx) % SIDE * SIDE + (place % SIDE + dy) % SIDE


def arrivals():
    xy = {(c, shift(p, n)): s for n in range(4) for s, (c, p) in enumerate(ORDER[n])}
    z = {}
    for n, sign in ((0, 1), (1, -1)):
        for s, (c, hop) in enumerate(Z_ORDER[n]):
            z[c, sign * (hop + 1) % CHIPS] = s
    return xy, z


XY_AT, Z_AT = arrivals()
BLOCK_AT = {p: max(XY_AT[c, p] for c in range(CHUNKS)) for p in range(1, SIDE * SIDE)} | {0: 0}
Z_LAG = 10
NEAR_AT = [(-1, 0), (4, 5), (8, 9), (11.5, 12.5), (13.6, 13.8)]


def kernel(
    v_hbm, tile_hbm, keep_hbm, thr_hbm, acc, scale_ref,
    row_panel, col_panel, loaded, tile_ref, keep_ref, thr_ref, colsum, stats, sums, psum,
    bulk_send, xy_recv, z_recv, pair_recv,
    detour_send, small_send, small_recv, load_sem, ready, hello,
):
    rows, cols = v_hbm.shape
    part = rows // CHUNKS
    order = rows * SIDE * SIDE
    me_row, me_col = lax.axis_index("row"), lax.axis_index("col")
    x, y = me_row // SIDE, me_row % SIDE
    z, core = me_col // CORES, me_col % CORES

    def xy_device(dx, dy):
        return {"row": (x + dx + SIDE) % SIDE * SIDE + (y + dy + SIDE) % SIDE}

    def z_device(dz, lane=0):
        return {"col": (z + dz + CHIPS) % CHIPS * CORES + (core if lane == 0 else 1 - core)}

    def load(q):
        spot = pl.ds(q * part, part)
        return pltpu.make_async_copy(v_hbm.at[spot], loaded.at[spot], load_sem.at[q])

    masks = (
        pltpu.make_async_copy(tile_hbm, tile_ref, load_sem.at[CHUNKS]),
        pltpu.make_async_copy(keep_hbm, keep_ref, load_sem.at[CHUNKS + 1]),
        pltpu.make_async_copy(thr_hbm, thr_ref, load_sem.at[CHUNKS + 2]),
    )
    masks[0].start()
    for q in range(CHUNKS):
        load(q).start()
    masks[1].start()
    masks[2].start()

    neighbours = [xy_device(*link) for link in LINKS] + [z_device(1), z_device(-1), z_device(0, 1)]
    later = [x < SIDE - 1, x == 0, y < SIDE - 1, y == 0, z < CHIPS - 1, z == 0, core == 1]
    barrier = pltpu.get_barrier_semaphore()
    earlier = 0
    for n, device in enumerate(neighbours):
        earlier = earlier + 1 - later[n].astype(jnp.int32)

        @pl.when(later[n])
        def _():
            pl.semaphore_signal(barrier, inc=1, device_id=device)


    def xy_copy(c, place, n):
        to = shift(place, n)
        return pltpu.make_async_remote_copy(
            src_ref=col_panel.at[pl.ds(place * rows + c * part, part)],
            dst_ref=col_panel.at[pl.ds(to * rows + c * part, part)],
            send_sem=bulk_send.at[0], recv_sem=xy_recv.at[XY_AT[c, to]],
            device_id=neighbours[n],
        )

    def z_copy(c, hop, n, sent=None, lo=0, count=part):
        sign = 1 - 2 * n
        spot = pl.ds(c * part + lo, count)
        to = sign * (hop + 1) % CHIPS
        return pltpu.make_async_remote_copy(
            src_ref=row_panel.at[sign * hop % CHIPS * CORES, spot],
            dst_ref=row_panel.at[to * CORES, spot],
            send_sem=bulk_send.at[1] if sent is None else sent, recv_sem=z_recv.at[Z_AT[c, to]],
            device_id=neighbours[4 + n],
        )

    def pair_copy(c, dz):
        spot = pl.ds(c * part, part)
        return pltpu.make_async_remote_copy(
            src_ref=row_panel.at[dz * CORES, spot], dst_ref=row_panel.at[dz * CORES + 1, spot],
            send_sem=bulk_send.at[1],
            recv_sem=pair_recv.at[CHIPS // 2 + 1 if Z_AT.get((c, dz)) == Z_SLOTS - 1 else min(dz, CHIPS - dz)],
            device_id=neighbours[6],
        )

    def send(n, s):
        if n < 4 and s < SLOTS:
            xy_copy(*ORDER[n][s], n).start()
        elif n == 6 and s < CHUNKS:
            pair_copy(s, 0).start()
        elif n in (4, 5) and s < Z_SLOTS:
            if n == 4 and Z_ORDER[0][s] == DETOUR:
                @pl.when(z != CHIPS - 1)
                def _():
                    z_copy(*DETOUR, 0, detour_send.at[0]).start()

                @pl.when(z == CHIPS - 1)
                def _():
                    z_copy(*DETOUR, 0, detour_send.at[0], 0, 32).start()
            else:
                z_copy(*Z_ORDER[n - 4][s], n - 4).start()

    @pl.when(earlier > 0)
    def _():
        pl.semaphore_wait(barrier, earlier)

    for n, device in enumerate(neighbours):
        @pl.when(jnp.logical_not(later[n]))
        def _():
            pl.semaphore_signal(ready.at[n ^ 1 if n < 6 else n], inc=1, device_id=device)

    masks[0].wait()
    stored = tile_ref[...].astype(jnp.float32)
    for q in range(CHUNKS):
        load(q).wait()
        for lo in range(q * part, (q + 1) * part, TB):
            for b in range(cols // TB):
                r, c = slice(lo, lo + TB), slice(b * TB, (b + 1) * TB)
                i = lo // TB
                factor = jnp.broadcast_to(stored[i : i + 1, b : b + 1], (EXTRA, TB)).astype(jnp.bfloat16)
                tile = loaded[r, c] * jnp.concatenate([factor] * (TB // EXTRA), axis=0)
                row_panel[0, r, c] = tile
                col_panel[r, c] = tile

    def when_not(n, do):
        @pl.when(jnp.logical_not(later[n]))
        def _():
            do()

    for s in range(AHEAD - 1):
        for n in range(6):
            when_not(n, lambda: send(n, s))
    def open_late(n):
        @pl.when(later[n])
        def _():
            with jax.named_scope(f"open{n}"):
                pl.semaphore_wait(ready.at[n], 1)
            for s in range(CHUNKS if n == 6 else AHEAD - (n != 5)):
                send(n, s)

    when_not(6, lambda: [send(6, s) for s in range(CHUNKS)])
    for n in (6, 0, 2, 4, 1, 3):
        open_late(n)

    def greet(k, over):
        for device in neighbours[4 * over : 4 + 3 * over]:
            pl.semaphore_signal(hello.at[2 * over + k % 2], inc=1, device_id=device)

    def greeted(k, over):
        pl.semaphore_wait(hello.at[2 * over + k % 2], 4 - over)

    greet(0, 0)

    def spread(buffer, k, count, device):
        def copy(d):
            return pltpu.make_async_remote_copy(
                src_ref=buffer.at[0], dst_ref=buffer.at[d],
                send_sem=small_send.at[0], recv_sem=small_recv.at[k], device_id=device(d),
            )

        everything = pltpu.make_async_remote_copy(
            src_ref=buffer.at[pl.ds(1, count - 1)], dst_ref=buffer.at[pl.ds(1, count - 1)],
            send_sem=small_send.at[0], recv_sem=small_recv.at[k], device_id=neighbours[6],
        )
        def far(d):
            return min(d // SIDE, SIDE - d // SIDE) + min(d % SIDE, SIDE - d % SIDE)

        return [copy(d) for d in sorted(range(1, count), key=far, reverse=True)], everything

    def by_row(d):
        return xy_device(d // SIDE, d % SIDE)

    def by_col(d):
        return z_device(d)

    column_sums, column_sums_all = spread(colsum, 0, SIDE * SIDE, by_row)

    total = jnp.zeros((1, cols), jnp.float32)
    for lo in range(0, rows, TB):
        block = col_panel[lo : lo + TB].astype(jnp.float32)
        total += jnp.sum(block, axis=0, keepdims=True)
    colsum[0] = total
    acc[...] = jnp.zeros((rows, cols), jnp.float32)
    psum[...] = jnp.zeros((EXTRA, cols), jnp.float32)
    with jax.named_scope("greet"):
        for k in range(3):
            greeted(k, 0)
            if k < 2:
                greet(k + 1, 0)
    for copy in column_sums:
        copy.start()
    for n in range(5):
        send(n, AHEAD - 1)
    when_not(5, lambda: send(5, AHEAD - 1))
    open_late(5)
    greet(0, 1)

    block_sums, block_sums_all = spread(stats, 1, CHIPS, by_col)

    def send_block_sums():
        column_sums_all.wait_recv()
        column_sums_all.wait_send()
        total = colsum[0]
        for i in range(1, SIDE * SIDE):
            total += colsum[i]
        stats[0] = total
        for copy in block_sums:
            copy.start()

    pair_sums = pltpu.make_async_remote_copy(
        src_ref=stats.at[pl.ds(0, CHIPS)], dst_ref=stats.at[pl.ds(CHIPS, CHIPS)],
        send_sem=small_send.at[0], recv_sem=small_recv.at[3], device_id=neighbours[6],
    )

    def pass_block_sums():
        block_sums_all.wait_recv()
        block_sums_all.wait_send()
        pair_sums.start()

    def take_block_sums():
        pair_sums.wait()
        line = lax.broadcasted_iota(jnp.int32, (EXTRA, cols), 0)

        @pl.loop(0, CHIPS * CORES)
        def _(i):
            rest, spot = stats[i], jnp.zeros((EXTRA, cols), jnp.float32)
            for k in range(3):
                term = rest.astype(jnp.bfloat16).astype(jnp.float32)
                rest = rest - term
                spot = jnp.where(line == k, jnp.broadcast_to(term, (EXTRA, cols)), spot)
            row_panel[i % CHIPS * CORES + i // CHIPS, rows:] = spot.astype(jnp.bfloat16)

    def inner(j):
        k = (x - j // SIDE + SIDE) % SIDE * SIDE + (y - j % SIDE + SIDE) % SIDE
        dz = (z - k // CORES + CHIPS) % CHIPS
        lane = (core + k) % CORES
        return dz, lane

    def near(dz, lane, step):
        there = None
        for side in range(CORES):
            reach = max([h for h in range(CHIPS // 2 + 1) if NEAR_AT[h][side] <= step], default=-1)
            one = (lane == side) & ((dz <= reach) | (dz >= CHIPS - reach))
            there = one if there is None else there | one
        return there

    def pick(i, values):
        found = values[0]
        for k, value in enumerate(values[1:], 1):
            found = found + (i == k).astype(jnp.int32) * (value - values[0])
        return found

    def met(of):
        dz, side = of
        k = (z - dz + CHIPS) % CHIPS * CORES + (core + side) % CORES
        return (x - k // SIDE + SIDE) % SIDE * SIDE + (y - k % SIDE + SIDE) % SIDE

    def multiply(blocks, summed):
        term = None
        for j in blocks:
            dz, lane = inner(j)
            left = row_panel[dz * CORES + lane] if summed else row_panel[dz * CORES + lane, :rows]
            right = col_panel[pl.ds(pl.multiple_of(j * rows, rows), rows)]
            one = jnp.dot(left, right, preferred_element_type=jnp.float32)
            term = one if term is None else term + one
        acc[...] += term[:rows]
        if summed:
            psum[...] += term[rows:]

    def multiply_those(found, summed):
        (first, one), (second, other) = found

        @pl.when(one & other)
        def _():
            multiply((first, second), summed)

        @pl.when(one ^ other)
        def _():
            multiply((jnp.where(one, first, second),), summed)

    def compute(step, before):
        fresh = [p for p in range(SIDE * SIDE) if p != LAST and before < BLOCK_AT[p] <= step]
        if len(fresh) == 2:
            multiply_those([(p, near(*inner(p), step)) for p in fresh], step > SUMMED)
        elif fresh:
            @pl.loop(0, len(fresh))
            def _(i):
                j = pick(i, fresh)

                @pl.when(near(*inner(j), step))
                def _():
                    multiply((j,), step > SUMMED)

        old = [p for p in range(SIDE * SIDE) if p != LAST and BLOCK_AT[p] <= before]
        came = [
            (dz, side) for side in range(CORES) for h in range(CHIPS // 2 + 1)
            for dz in sorted({h, (CHIPS - h) % CHIPS}) if before < NEAR_AT[h][side] <= step
        ]
        def there(of):
            j = met(of)
            here = j == old[0]
            for p in old[1:]:
                here = here | (j == p)
            return j, here

        if old and len(came) == 2:
            multiply_those([there(of) for of in came], step > SUMMED)
        elif old and came:
            @pl.loop(0, len(came))
            def _(i):
                dz = pick(i, [c[0] for c in came])
                side = pick(i, [c[1] for c in came])
                j, here = there((dz, side))

                @pl.when(here)
                def _():
                    multiply((j,), step > SUMMED)

    def add_sums(step):
        fresh = [p for p in range(SIDE * SIDE) if BLOCK_AT[p] <= step]

        @pl.loop(0, len(fresh))
        def _(i):
            j = pick(i, fresh)
            dz, lane = inner(j)

            @pl.when(near(dz, lane, step))
            def _():
                block = col_panel[pl.ds(pl.multiple_of(j * rows, rows), rows)]
                psum[...] += jnp.dot(
                    row_panel[dz * CORES + lane, rows:], block, preferred_element_type=jnp.float32
                )

    def await_rows(count, sem):
        spot = col_panel.at[pl.ds(0, count)]
        pltpu.make_async_remote_copy(
            src_ref=spot, dst_ref=spot, send_sem=bulk_send.at[0], recv_sem=sem, device_id=neighbours[0]
        ).wait_recv()

    def take_xy(s):
        await_rows(4 * part, xy_recv.at[s])

    def take_z(s):
        if s < Z_SLOTS:
            await_rows(2 * part, z_recv.at[s])
            for (c, dz), at in sorted(Z_AT.items()):
                if at == s:
                    pair_copy(c, dz).start()

    def take_pair(h):
        await_rows(rows // 2 if h >= CHIPS // 2 else rows if h == 0 else 2 * rows, pair_recv.at[h])

    before = -1
    for s in range(SLOTS - 1):
        if s < SLOTS - 1:
            if s == Z_SLOTS - 1:
                with jax.named_scope(f"z{s}"):
                    take_z(s)
            with jax.named_scope(f"xy{s}"):
                take_xy(s)
            for n in range(4):
                send(n, s + AHEAD)
        if 0 < s <= Z_LAG:
            with jax.named_scope(f"z{s - 1}"):
                take_z(s - 1)
        for n in (4, 5):
            if s > 0:
                send(n, s + AHEAD - 1)
        for h in range(CHIPS // 2):
            if s == NEAR_AT[h][1]:
                with jax.named_scope(f"pair{h}"):
                    take_pair(h)
        with jax.named_scope(f"sums{s}"):
            if s < 3:
                greeted(s, 1)
                if s < 2:
                    greet(s + 1, 1)
            if s == 3:
                send_block_sums()
            if s == SUMMED - 1:
                pass_block_sums()
            if s == SUMMED:
                take_block_sums()
                add_sums(before)
        if s in POINTS:
            with jax.named_scope(f"multiply{s}"):
                compute(s, before)
            before = s
        if s == Z_SLOTS - 2:
            with jax.named_scope("pair3"):
                take_pair(CHIPS // 2 - 1)
            with jax.named_scope("multiply3b"):
                compute(NEAR_AT[-2][1], before)
            before = NEAR_AT[-2][1]
        if Z_LAG <= s < Z_SLOTS - 1:
            with jax.named_scope(f"z{s}"):
                take_z(s)
            if s == Z_AT[DETOUR[0], CHIPS - DETOUR[1]]:
                @pl.when(z == 1)
                def _():
                    z_copy(*DETOUR, 1, detour_send.at[1], 32, part - 32).start()

    near_last = met((CHIPS // 2, 0))
    with jax.named_scope("multiplyA"):
        @pl.when((core == 1) & (near_last != LAST))
        def _():
            multiply((near_last,), True)

    masks[1].wait()
    masks[2].wait()
    kept = keep_ref[...].astype(jnp.float32)
    level = 0.125 * thr_ref[...].astype(jnp.float32)
    far = met((CHIPS // 2, 1))
    for turn in range(CORES):
        with jax.named_scope(f"last{turn}"):
            @pl.when(core == turn)
            def _():
                take_pair(CHIPS // 2)
                if turn == 0:
                    take_pair(CHIPS // 2 + 1)

            @pl.when(core != turn)
            def _():
                take_xy(SLOTS - 1)
        if turn == 0:
            multiply_those([
                (near_last, (core == 0) & (near_last != LAST)),
                ((1 - core) * far + core * LAST, far != LAST),
            ], True)
    final = core * far + (1 - core) * LAST
    dz, lane = inner(final)
    slot = dz * CORES + lane
    block = col_panel[pl.ds(pl.multiple_of(final * rows, rows), rows)]
    lines = psum[...] + jnp.dot(row_panel[slot, rows:], block, preferred_element_type=jnp.float32)
    cut = level * ((lines[2:3] + lines[1:2] + lines[0:1]) / order)
    parts = [jnp.zeros((1, TB), jnp.float32) for _ in range(cols // TB)]
    late = sorted(c for c in range(CHUNKS) if Z_AT[c, CHIPS // 2] == Z_SLOTS - 1)
    for q in sorted(range(CHUNKS), key=lambda c: c in late):
        if q == late[0]:
            with jax.named_scope("last2"):
                @pl.when(core == 1)
                def _():
                    take_pair(CHIPS // 2 + 1)
        lo = q * TB
        term = jnp.dot(row_panel[slot, lo : lo + TB], block, preferred_element_type=jnp.float32)
        for b in range(cols // TB):
            r, c = slice(lo, lo + TB), slice(b * TB, (b + 1) * TB)
            keep = jnp.broadcast_to(kept[lo // TB : lo // TB + 1, b : b + 1], (TB, TB))
            pruned = jnp.maximum(acc[r, c] + term[:, c] - cut[:, c], 0.0) * keep
            acc[r, c] = pruned
            parts[b] += jnp.sum(pruned, axis=0, keepdims=True)
    sums[0] = jnp.concatenate(parts, axis=1)

    totals, totals_all = spread(sums, 2, SIDE * SIDE, by_row)
    for copy in totals:
        copy.start()

    for k, count in enumerate((4 * SLOTS * part, (2 * Z_SLOTS - 1) * part + CHIPS * rows)):
        spot = col_panel.at[pl.ds(0, count)]
        pltpu.make_async_remote_copy(
            src_ref=spot, dst_ref=spot, send_sem=bulk_send.at[k], recv_sem=bulk_send.at[k],
            device_id=neighbours[0],
        ).wait_send()

    for n, sends, count in ((0, z != CHIPS - 1, part), (0, z == CHIPS - 1, 32), (1, z == 1, part - 32)):
        @pl.when(sends)
        def _():
            z_copy(*DETOUR, n, detour_send.at[n], 0, count).wait_send()

    with jax.named_scope("totals"):
        totals_all.wait_send()
        totals_all.wait_recv()
    total = sums[0]
    for i in range(1, SIDE * SIDE):
        total += sums[i]
    scale_ref[...] = 1.0 / jnp.maximum(total / order, 0.1)


def on_device(values, tile_mask, keep_mask, thr_index):
    rows, cols = values.shape
    dma, plain = pltpu.SemaphoreType.DMA, pltpu.SemaphoreType.REGULAR
    vmem, anywhere = pl.BlockSpec(memory_space=pltpu.VMEM), pl.BlockSpec(memory_space=pl.ANY)
    blocks = SIDE * SIDE
    pruned, scale = pl.pallas_call(
        kernel,
        out_shape=(pltpu.VMEM((rows, cols), jnp.float32), pltpu.VMEM((1, cols), jnp.float32)),
        in_specs=[anywhere] * 4,
        out_specs=(vmem, vmem),
        scratch_shapes=[
            pltpu.VMEM((CHIPS * CORES, rows + EXTRA, cols), jnp.bfloat16),
            pltpu.VMEM((blocks * rows, cols), jnp.bfloat16),
            pltpu.VMEM((rows, cols), jnp.bfloat16),
            pltpu.VMEM(tile_mask.shape, jnp.int32),
            pltpu.VMEM(keep_mask.shape, jnp.int32),
            pltpu.VMEM((1, cols), jnp.int32),
            pltpu.VMEM((blocks, 1, cols), jnp.float32),
            pltpu.VMEM((CHIPS * CORES, 1, cols), jnp.float32),
            pltpu.VMEM((blocks, 1, cols), jnp.float32),
            pltpu.VMEM((EXTRA, cols), jnp.float32),
            dma((2,)),
            dma((SLOTS,)),
            dma((Z_SLOTS,)),
            dma((CHIPS // 2 + 2,)),
            dma((2,)),
            dma((1,)),
            dma((4,)),
            dma((CHUNKS + 3,)),
            plain((7,)),
            plain((4,)),
        ],
        compiler_params=pltpu.CompilerParams(
            collective_id=0, has_side_effects=True,
            vmem_limit_bytes=63 * 2**20 - 4 * rows * cols + 2**19,
        ),
    )(values, tile_mask, keep_mask, thr_index.reshape(1, cols))
    return (pruned * scale).astype(jnp.bfloat16)


def solution(mesh):
    return jax.shard_map(
        on_device,
        mesh=mesh,
        in_specs=(P("row", "col"), P("row", "col"), P("row", "col"), P("col")),
        out_specs=P("row", "col"),
        check_vma=False,
    )
```
